512 devices in a mesh: fsdp: 32 (over z, x_hi), pipe: 2 (over core), dp: 8 (over x_lo, y).
Axes of the slice: x: 4 (x_hi: 2, x_lo: 2; x = x_hi * 2 + x_lo), y: 4, z: 16, core: 2. Of those that a mesh axis runs over, the one named last changes fastest.
Arguments:
- video_tokens: bfloat16 [8, 4096, 2560], P('dp', 'fsdp'), may hold values from -6 to 6
- cached_out: bfloat16 [2, 8, 4096, 2560], P('pipe', 'dp', 'fsdp'), may hold values from -6 to 6
- fresh_mask: int32 [2, 8, 4096], P('pipe', 'dp', 'fsdp'), may hold values from 0 to 1, as said below
- timestep: int32 [8], P('dp'), may hold values from 0 to 49
- up_weight: bfloat16 [2, 7168, 2560], P('pipe', 'fsdp'), may hold values from -0.125 to 0.125
- down_weight: bfloat16 [2, 7168, 2560], P('pipe', 'fsdp'), may hold values from -0.0625 to 0.0625
- router_in: bfloat16 [2, 2560, 256], P('pipe', 'fsdp'), may hold values from -0.125 to 0.125
- router_bias: float32 [2, 50, 256], P('pipe'), may hold values from -6 to 6
- router_out: float32 [2, 256], P('pipe'), may hold values from -0.375 to 0.375
- out_cotangent: bfloat16 [8, 4096, 2560], P('dp', 'fsdp'), may hold values from -0.119628906 to 0.119628906
Outputs:
- blended: bfloat16 [2, 8, 4096, 2560], P('pipe', 'dp', 'fsdp')
- grad_router_in: float32 [2, 2560, 256], P('pipe', 'fsdp')
- grad_router_bias: float32 [2, 50, 256], P('pipe')
- grad_router_out: float32 [2, 256], P('pipe')
The draws below stay inside these ranges and needn't reach their ends.
Inputs may be any that keep to these rules, and one draw needn't show every extreme that they name: `fresh_mask`: for each section and video, the 128 consecutive tokens of one index of fsdp hold 1 to 2 ones, and some index holds exactly 2.
All inputs are finite; a program needn't handle non-finite values.
Results may differ from the reference program's by a relative error of at most 0.023.
Values may be sent and summed in bfloat16 or wider, within the bound.
No kernel may reach another device: no remote copies, remote signals or barrier semaphores. Data moves between devices by JAX's collectives and lax.ppermute only.
A program may use at most 64 MiB of HBM per device.

```python
import jax
import jax.numpy as jnp
from jax import lax

D = 2560
FF = 7168
RH = 256
STEPS = 50
FRESH = 2
TOK_DEV = 128
TOKENS = 4096
VIDEOS = 8
N_FSDP = 32
N_DP = 8


def draw_fresh_mask(key, part):
    block_count = TOKENS // TOK_DEV
    key_count = jax.random.fold_in(key, 11)
    key_full = jax.random.fold_in(key, 12)
    key_order = jax.random.fold_in(key, 13)
    counts = jax.random.randint(key_count, (2, VIDEOS, block_count), FRESH // 2, FRESH + 1)
    full_block = jax.random.randint(key_full, (2, VIDEOS), 0, block_count)
    counts = jnp.where(jnp.arange(block_count)[None, None, :] == full_block[:, :, None], FRESH, counts)
    scores = jax.random.randint(key_order, (2, VIDEOS, block_count, TOK_DEV), 0, 1 << 20) * TOK_DEV + jnp.arange(TOK_DEV)[None, None, None, :]
    ranks = jnp.argsort(jnp.argsort(scores, axis=3), axis=3)
    chosen = (ranks < counts[:, :, :, None]).astype(jnp.int32)
    return chosen.reshape(2, VIDEOS, TOKENS)


def touch_ends(entries, key, smallest, largest):
    shape = entries.shape
    spot = [jax.random.randint(jax.random.fold_in(key, axis), (), 0, shape[axis]) for axis in range(len(shape))]
    entries = entries.at[tuple(spot)].set(smallest)
    longest = shape.index(max(shape))
    spot[longest] = (spot[longest] + 1) % shape[longest]
    return entries.at[tuple(spot)].set(largest)


def levels(key, extent, pieces, smallest, largest):
    level, own = 1.0, jax.random.fold_in(key, 6)
    for dim, blocks in pieces:
        draws = jnp.exp(jax.random.uniform(jax.random.fold_in(own, dim), (blocks,), jnp.float32, smallest / len(pieces), largest / len(pieces)))
        level = level * jnp.repeat(draws, extent[dim] // blocks).reshape([-1 if axis == dim else 1 for axis in range(len(extent))])
    return level


def bell_draw(own_key, extent, deviation, bound, pieces=(), kind=jnp.bfloat16):
    result = jax.random.normal(own_key, extent, jnp.float32) * deviation
    if len(pieces) > 0:
        result = levels(own_key, extent, pieces, -0.22, 0.18) * result
    return jnp.clip(result, min=-bound, max=bound).astype(kind)


def setup_inputs(seed: int = 0) -> dict:
    splits = jax.random.split(jax.random.key(seed), 11)
    video_tokens = bell_draw(splits[0], (VIDEOS, TOKENS, D), 1.0, 6.0, ((0, 8), (1, 32)))
    cached_out = bell_draw(splits[1], (2, VIDEOS, TOKENS, D), 1.0, 6.0, ((0, 2), (1, 8), (2, 32)))
    fresh_mask = draw_fresh_mask(jax.random.fold_in(splits[10], 71), 0)
    timestep = touch_ends(jax.random.randint(splits[3], (VIDEOS,), 0, STEPS), jax.random.fold_in(splits[3], 1), 0, STEPS - 1).astype(jnp.int32)
    up_weight = bell_draw(splits[4], (2, FF, D), D ** -0.5, 0.125, ((0, 2), (1, 32)))
    down_weight = bell_draw(splits[5], (2, FF, D), FF ** -0.5, 0.0625, ((0, 2), (1, 32)))
    router_in = bell_draw(splits[6], (2, D, RH), D ** -0.5, 0.125, ((0, 2), (1, 32)))
    router_bias = bell_draw(splits[7], (2, STEPS, RH), 1.0, 6.0, ((0, 2),), jnp.float32)
    router_out = bell_draw(splits[8], (2, RH), RH ** -0.5, 0.375, ((0, 2),), jnp.float32)
    out_cotangent = bell_draw(splits[9], (VIDEOS, TOKENS, D), 0.02, 0.119628906, ((0, 8), (1, 32)))
    return {"video_tokens": video_tokens, "cached_out": cached_out, "fresh_mask": fresh_mask, "timestep": timestep, "up_weight": up_weight, "down_weight": down_weight, "router_in": router_in, "router_bias": router_bias, "router_out": router_out, "out_cotangent": out_cotangent}


layer_eps = 1e-06
gelu_scale = 0.7978845608028654
gelu_cubic = 0.044715

def gelu_tanh(values):
    inner_arg = gelu_scale * (values + gelu_cubic * values * values * values)
    return 0.5 * values * (1.0 + jnp.tanh(inner_arg))

def gelu_slope(values):
    inner_arg = gelu_scale * (values + gelu_cubic * values * values * values)
    tanh_val = jnp.tanh(inner_arg)
    return 0.5 * (1.0 + tanh_val) + 0.5 * values * (1.0 - tanh_val * tanh_val) * gelu_scale * (1.0 + 3.0 * gelu_cubic * values * values)

def normalize(inputs):
    values = inputs.astype(jnp.float32)
    center = values - lax.optimization_barrier(jnp.mean(values, axis=1, keepdims=True))
    inv_std = lax.rsqrt(lax.optimization_barrier(jnp.mean(center * center, axis=1, keepdims=True)) + layer_eps)
    return (center * inv_std, inv_std)

def normalize_back(scaled, inv_std, grads):
    return inv_std * (grads - lax.optimization_barrier(jnp.mean(grads, axis=1, keepdims=True)) - scaled * lax.optimization_barrier(jnp.mean(grads * scaled, axis=1, keepdims=True)))

def pack_index(mask_row):
    blocks_mask = mask_row.reshape(N_FSDP, TOK_DEV)
    order = jnp.argsort(1 - blocks_mask, axis=1, stable=True)[:, :FRESH].astype(jnp.int32)
    index = order + (jnp.arange(N_FSDP, dtype=jnp.int32) * TOK_DEV)[:, None]
    live = (jnp.arange(FRESH)[None, :] < lax.optimization_barrier(jnp.sum(blocks_mask, axis=1))[:, None]).astype(jnp.float32)
    return (index.reshape(-1).astype(jnp.int32), live.reshape(-1))

def block_terms(left, weight):
    rows = left.shape[0]
    parts = jnp.transpose(left.reshape(rows, N_FSDP, FF // N_FSDP), (1, 0, 2))
    weight_parts = weight.reshape(N_FSDP, FF // N_FSDP, D)

    def one_block(pair):
        return jnp.dot(pair[0], pair[1], preferred_element_type=jnp.float32)
    return lax.map(one_block, (parts, weight_parts))

def section_forward(rows_in, cached_rows, live_rows, bias_row, w_up, w_down, r_in, r_out):
    scaled, inv_std = normalize(rows_in)
    normed = scaled.astype(jnp.bfloat16)
    pre_act = jnp.dot(normed, w_up.T, preferred_element_type=jnp.float32)
    hid_act = gelu_tanh(pre_act).astype(jnp.bfloat16)
    blocks = block_terms(hid_act, w_down)
    block_sum = lax.optimization_barrier(jnp.sum(blocks.astype(jnp.bfloat16).astype(jnp.float32), axis=0))
    fresh_out = rows_in.astype(jnp.float32) + block_sum
    router_pre = jnp.dot(normed, r_in, preferred_element_type=jnp.float32) + bias_row[None, :]
    gate = jax.nn.sigmoid(jnp.dot(gelu_tanh(router_pre), r_out, precision=lax.Precision.HIGHEST))
    delta = live_rows[:, None] * gate[:, None] * (fresh_out - cached_rows)
    return (delta, (scaled, inv_std, normed, pre_act, router_pre, gate, fresh_out, cached_rows))

def router_back(stored, live_rows, cotangent, r_out):
    scaled, inv_std, normed, pre_act, router_pre, gate, fresh_out, cached_f = stored
    gate_grad = lax.optimization_barrier(jnp.sum(cotangent * live_rows[:, None] * (fresh_out - cached_f), axis=1))
    fresh_grad = cotangent * (live_rows * gate)[:, None]
    logit_grad = gate_grad * gate * (1.0 - gate)
    out_grad = jnp.dot(logit_grad, gelu_tanh(router_pre), precision=lax.Precision.HIGHEST)
    hidden_grad = logit_grad[:, None] * r_out[None, :] * gelu_slope(router_pre)
    hidden_b = hidden_grad.astype(jnp.bfloat16)
    in_grad = jnp.dot(normed.T, hidden_b, preferred_element_type=jnp.float32)
    bias_sum = lax.optimization_barrier(jnp.sum(hidden_grad, axis=0))
    return (fresh_grad, hidden_b, in_grad, bias_sum, out_grad)

def block_back(stored, fresh_grad, hidden_b, w_up, w_down, r_in):
    scaled, inv_std, normed, pre_act, router_pre, gate, fresh_out, cached_f = stored
    rows = fresh_grad.shape[0]
    fresh_b = fresh_grad.astype(jnp.bfloat16)
    act_grad = jnp.dot(fresh_b, w_down.T, preferred_element_type=jnp.float32)
    pre_grad = (act_grad * gelu_slope(pre_act)).astype(jnp.bfloat16)
    blocks = block_terms(pre_grad, w_up)
    router_term = jnp.dot(hidden_b, r_in.T, preferred_element_type=jnp.float32)
    placed = router_term.reshape(rows, N_FSDP, D // N_FSDP)[None] * jnp.eye(N_FSDP, dtype=jnp.float32)[:, None, :, None]
    blocks = blocks + placed.reshape(N_FSDP, rows, D)
    normed_grad = lax.optimization_barrier(jnp.sum(blocks.astype(jnp.bfloat16).astype(jnp.float32), axis=0))
    return fresh_grad + normalize_back(scaled, inv_std, normed_grad)

def reference(video_tokens, cached_out, fresh_mask, timestep, up_weight, down_weight, router_in, router_bias, router_out, out_cotangent):
    first_out = []
    second_out = []
    in_grads = [jnp.zeros((D, RH), jnp.float32), jnp.zeros((D, RH), jnp.float32)]
    bias_grads = [jnp.zeros((STEPS, RH), jnp.float32), jnp.zeros((STEPS, RH), jnp.float32)]
    out_grads = [jnp.zeros((RH,), jnp.float32), jnp.zeros((RH,), jnp.float32)]
    for video_index in range(N_DP):
        hot_step = (jnp.arange(STEPS) == timestep[video_index]).astype(jnp.float32)
        bias_first = jnp.dot(hot_step, router_bias[0], precision=lax.Precision.HIGHEST)
        bias_second = jnp.dot(hot_step, router_bias[1], precision=lax.Precision.HIGHEST)
        index_first, live_first = pack_index(fresh_mask[0, video_index])
        index_second, live_second = pack_index(fresh_mask[1, video_index])
        cached_first = cached_out[0, video_index].astype(jnp.float32)
        cached_second = cached_out[1, video_index].astype(jnp.float32)
        delta_first, stored_first = section_forward(video_tokens[video_index][index_first], cached_first[index_first], live_first, bias_first, up_weight[0], down_weight[0], router_in[0], router_out[0])
        out_first = cached_first.at[index_first].add(delta_first).astype(jnp.bfloat16)
        delta_second, stored_second = section_forward(out_first[index_second], cached_second[index_second], live_second, bias_second, up_weight[1], down_weight[1], router_in[1], router_out[1])
        out_second = cached_second.at[index_second].add(delta_second).astype(jnp.bfloat16)
        cot_second = out_cotangent[video_index].astype(jnp.float32)[index_second]
        fresh_grad, hidden_b, in_second, bias_second_sum, out_second_grad = router_back(stored_second, live_second, cot_second, router_out[1])
        input_grad = block_back(stored_second, fresh_grad, hidden_b, up_weight[1], down_weight[1], router_in[1])
        full_grad = jnp.zeros((TOKENS, D), jnp.float32).at[index_second].add(input_grad)
        cot_first = full_grad[index_first]
        unused_grad, unused_hidden, in_first, bias_first_sum, out_first_grad = router_back(stored_first, live_first, cot_first, router_out[0])
        in_grads = [in_grads[0] + in_first, in_grads[1] + in_second]
        bias_grads = [bias_grads[0] + hot_step[:, None] * bias_first_sum[None, :], bias_grads[1] + hot_step[:, None] * bias_second_sum[None, :]]
        out_grads = [out_grads[0] + out_first_grad, out_grads[1] + out_second_grad]
        first_out.append(out_first)
        second_out.append(out_second)
    blended = jnp.stack([jnp.stack(first_out), jnp.stack(second_out)])
    return (blended, jnp.stack(in_grads), jnp.stack(bias_grads), jnp.stack(out_grads))
```

```python
import jax
import jax.numpy as jnp
from jax import lax
from jax.sharding import Mesh
from jax.sharding import PartitionSpec as P


FSDP = ("fsdp_0", "fsdp_1")
PLANE = ("fsdp_1", "dp")


layer_eps = 1e-06
gelu_scale = 0.7978845608028654
gelu_cubic = 0.044715


def from_everyone(value, axis):
    copies = jnp.broadcast_to(value, (lax.axis_size(axis), *value.shape))
    arrived = lax.all_to_all(copies, axis, split_axis=0, concat_axis=0, tiled=True)
    return arrived.reshape(-1, value.shape[-1])


def summed_on_arrival(value, axis):
    blocks = value.reshape(lax.axis_size(axis), -1, value.shape[-1])
    arrived = lax.all_to_all(blocks, axis, split_axis=0, concat_axis=0, tiled=True)
    return arrived.astype(jnp.float32).sum(axis=0)


def gelu_both(values):
    inner_arg = gelu_scale * (values + gelu_cubic * values * values * values)
    tanh_val = jnp.tanh(inner_arg)
    half = 0.5 * (1.0 + tanh_val)
    slope = half + 0.5 * values * (1.0 - tanh_val * tanh_val) * gelu_scale * (
        1.0 + 3.0 * gelu_cubic * values * values
    )
    return (values * half, slope)


def normalize(inputs):
    values = inputs.astype(jnp.float32)
    center = values - jnp.mean(values, axis=1, keepdims=True)
    inv_std = lax.rsqrt(jnp.mean(center * center, axis=1, keepdims=True) + layer_eps)
    return (center * inv_std, inv_std)


def contract_last(left, right):
    return lax.dot_general(
        left, right, (((1,), (1,)), ((), ())), preferred_element_type=jnp.float32
    )


def contract_first(left, right):
    return lax.dot_general(
        left, right, (((0,), (0,)), ((), ())), preferred_element_type=jnp.float32
    )


def times(left, right):
    return jnp.dot(left, right, preferred_element_type=jnp.float32)


def fresh_positions(mask_row):
    rows = mask_row.shape[0]
    places = jnp.arange(rows)
    fresh = mask_row > 0
    first = jnp.min(jnp.where(fresh, places, rows))
    second = jnp.min(jnp.where(fresh & (places != first), places, rows))
    has_second = second < rows
    second = jnp.where(has_second, second, (first + 1) % rows)
    live = jnp.stack([jnp.float32(1.0), has_second.astype(jnp.float32)])
    return (first, second, live)


def rows_at(values, first, second):
    return jnp.concatenate(
        [lax.dynamic_slice_in_dim(values, first, 1), lax.dynamic_slice_in_dim(values, second, 1)]
    )


def body(
    video_tokens,
    cached_out,
    fresh_mask,
    timestep,
    up_weight,
    down_weight,
    router_in,
    router_bias,
    router_out,
    out_cotangent,
):
    second_section = lax.axis_index("pipe") == 1
    near = lax.axis_index("fsdp_1")
    along = lax.axis_index("fsdp_0")
    column_slot = lax.axis_index(FSDP)
    cached = cached_out[0, 0]
    w_up = up_weight[0]
    w_down = down_weight[0]
    r_in = router_in[0]
    r_out = router_out[0]
    features = cached.shape[1]
    hidden = r_in.shape[1]
    shard_cols = r_in.shape[0]
    near_count = lax.axis_size("fsdp_1")
    bias_row = lax.dynamic_slice_in_dim(router_bias[0], timestep[0], 1)

    swap = [(1, 3), (3, 1)]
    other_up = lax.ppermute(w_up, ("fsdp_1", "pipe"), swap)
    other_down = lax.ppermute(w_down, ("fsdp_1", "pipe"), swap)
    other_in = lax.ppermute(r_in, ("fsdp_1", "pipe"), swap)

    first, second, live = fresh_positions(fresh_mask[0, 0])
    live = live[:, None]
    positions = jnp.stack([first, second]).astype(jnp.float32)
    asked = lax.ppermute(positions, "pipe", [(1, 0)]).astype(jnp.int32)
    match = (asked[:, None] == positions.astype(jnp.int32)[None, :]).astype(jnp.float32)
    match = match * live[:, 0][None, :]

    rows_cached = rows_at(cached, first, second).astype(jnp.float32)
    cot_rows = rows_at(out_cotangent[0], first, second)
    scaled_first, _ = normalize(rows_at(video_tokens[0], first, second))
    rows_first = rows_at(video_tokens[0], first, second).astype(jnp.float32)
    sent_first = jnp.where(second_section, cot_rows, scaled_first.astype(jnp.bfloat16))

    def gate_of(router_pre):
        value, slope = gelu_both(router_pre)
        gate = jax.nn.sigmoid(jnp.sum(value * r_out[None, :], axis=1, keepdims=True))
        return (value, slope, gate)

    gathered = from_everyone(sent_first, FSDP)
    act_first, _ = gelu_both(contract_last(gathered, w_up))
    terms = times(act_first.astype(jnp.bfloat16), w_down)
    columns = lax.dynamic_slice_in_dim(gathered, column_slot * shard_cols, shard_cols, 1)
    sums_first = summed_on_arrival(
        jnp.concatenate([terms, times(columns, r_in)], axis=1).astype(jnp.bfloat16), FSDP
    )
    value_first, slope_first, gate_first = gate_of(sums_first[:, features:] + bias_row)
    change_first = rows_first + sums_first[:, :features] - rows_cached
    added_first = live * gate_first * change_first

    cached_asked = rows_at(cached, asked[0], asked[1]).astype(jnp.float32)

    def at_asked(values):
        return match[:, :1] * values[:1] + match[:, 1:] * values[1:]

    passed = jnp.concatenate([cached_asked + at_asked(added_first), at_asked(change_first)])
    passed = lax.ppermute(passed.astype(jnp.bfloat16), "pipe", [(0, 1)])
    rows_second = passed[:2]
    moved = passed[2:].astype(jnp.float32)

    scaled, inv_std = normalize(rows_second)
    tangent = inv_std * (
        moved
        - jnp.mean(moved, axis=1, keepdims=True)
        - scaled * jnp.mean(moved * scaled, axis=1, keepdims=True)
    )
    both = jnp.concatenate([scaled, tangent], axis=1).astype(jnp.bfloat16)
    both = from_everyone(both, "fsdp_0")
    group_rows = both.shape[0]
    normed_group = both[:, :features]
    stacked = jnp.concatenate([normed_group, both[:, features:]])
    up_pair = jnp.concatenate([w_up, other_up])
    down_pair = jnp.concatenate([w_down, other_down])
    in_pair = jnp.where(
        near == 0, jnp.concatenate([r_in, other_in]), jnp.concatenate([other_in, r_in])
    )
    by_near = gathered.reshape(-1, near_count, 2, features)
    group_first = lax.dynamic_index_in_dim(by_near, near, 1, keepdims=False)
    group_first = group_first.reshape(group_rows, features)
    act_grad = contract_last(group_first, down_pair)
    pre_both = contract_last(stacked, up_pair)
    act, act_slope = gelu_both(pre_both[:group_rows])
    terms = times(act.astype(jnp.bfloat16), down_pair)
    slope_terms = jnp.sum(act_grad * act_slope * pre_both[group_rows:], axis=1, keepdims=True)
    pair_cols = near_count * shard_cols
    routed = times(
        lax.dynamic_slice_in_dim(stacked, along * pair_cols, pair_cols, 1), in_pair
    )
    sums = summed_on_arrival(
        jnp.concatenate(
            [
                terms,
                routed[:group_rows],
                routed[group_rows:],
                jnp.broadcast_to(slope_terms, (group_rows, 128)),
            ],
            axis=1,
        ).astype(jnp.bfloat16),
        "fsdp_0",
    )
    value, slope, gate = gate_of(sums[:, features : features + hidden] + bias_row)
    change = rows_second.astype(jnp.float32) + sums[:, :features] - rows_cached
    added = live * gate * change
    cot = cot_rows.astype(jnp.float32)
    gate_grad = live * jnp.sum(cot * change, axis=1, keepdims=True)
    logit_grad = gate_grad * gate * (1.0 - gate)
    routed_tangent = sums[:, features + hidden : features + 2 * hidden]
    input_grad = live * gate * (
        jnp.sum(cot * moved, axis=1, keepdims=True) + sums[:, features + 2 * hidden :][:, :1]
    ) + logit_grad * jnp.sum(r_out[None, :] * slope * routed_tangent, axis=1, keepdims=True)

    returned = lax.ppermute(input_grad[:, 0], "pipe", [(1, 0)])
    gate_grad_first = jnp.sum(match * returned[:, None], axis=0)[:, None]
    logit_grad_first = gate_grad_first * gate_first * (1.0 - gate_first)

    logit_own = jnp.where(second_section, logit_grad, logit_grad_first)
    slope_own = jnp.where(second_section, slope, slope_first)
    value_own = jnp.where(second_section, value, value_first)
    late = jnp.concatenate([logit_own * r_out[None, :] * slope_own, logit_own * value_own], axis=1)
    late = from_everyone(late.astype(jnp.bfloat16), "fsdp_0")
    normed_own = jnp.where(second_section, normed_group, group_first)
    pair_columns = lax.dynamic_slice_in_dim(normed_own, along * pair_cols, pair_cols, 1)
    in_grad = contract_first(pair_columns, late[:, :hidden])
    totals = jnp.sum(late.astype(jnp.float32), axis=0).reshape(2, hidden)
    step_row = jnp.broadcast_to(timestep[0].astype(jnp.float32), (1, hidden))
    dp_count = lax.axis_size("dp")
    extra = jnp.concatenate([totals, step_row])
    message = jnp.concatenate(
        [
            in_grad.reshape(near_count, shard_cols, hidden),
            jnp.broadcast_to(extra, (near_count, *extra.shape)),
        ],
        axis=1,
    ).astype(jnp.bfloat16)
    message = jnp.broadcast_to(message[:, None], (near_count, dp_count, *message.shape[1:]))
    arrived = lax.all_to_all(
        message.reshape(-1, *message.shape[2:]), PLANE, split_axis=0, concat_axis=0, tiled=True
    ).astype(jnp.float32)
    summed_in = jnp.sum(arrived[:, :shard_cols], axis=0)
    bias_parts = arrived[:, shard_cols]
    summed_out = jnp.sum(arrived[:, shard_cols + 1], axis=0)
    steps = jnp.arange(router_bias.shape[1]).astype(jnp.float32)
    is_step = steps[:, None] == arrived[:, shard_cols + 2, 0][None, :]
    summed_bias = jnp.sum(jnp.where(is_step[:, :, None], bias_parts[None], 0.0), axis=1)

    new_rows = rows_cached + jnp.where(second_section, added, added_first)
    new_rows = new_rows.astype(jnp.bfloat16)
    blended = lax.dynamic_update_slice_in_dim(cached, new_rows[:1], first, 0)
    blended = lax.dynamic_update_slice_in_dim(blended, new_rows[1:], second, 0)
    return (blended[None, None], summed_in[None], summed_bias[None], summed_out[None])


def solution(mesh):
    torus = Mesh(
        mesh.devices.reshape(16, 2, mesh.shape["pipe"], mesh.shape["dp"]),
        ("fsdp_0", "fsdp_1", "pipe", "dp"),
    )
    return jax.shard_map(
        body,
        mesh=torus,
        in_specs=(
            P("dp", FSDP, None),
            P("pipe", "dp", FSDP, None),
            P("pipe", "dp", FSDP),
            P("dp"),
            P("pipe", FSDP, None),
            P("pipe", FSDP, None),
            P("pipe", FSDP, None),
            P("pipe", None, None),
            P("pipe", None),
            P("dp", FSDP, None),
        ),
        out_specs=(
            P("pipe", "dp", FSDP, None),
            P("pipe", FSDP, None),
            P("pipe", None, None),
            P("pipe", None),
        ),
        check_vma=False,
    )
```

```python
import jax
import jax.numpy as jnp
from jax import lax
from jax.sharding import Mesh
from jax.sharding import PartitionSpec as P

FRESH = 2
FSDP = ("fsdp_0", "fsdp_1")
PLANE = ("fsdp_1", "dp")


layer_eps = 1e-06
gelu_scale = 0.7978845608028654
gelu_cubic = 0.044715


def from_everyone(value, axis):
    copies = jnp.broadcast_to(value, (lax.axis_size(axis), *value.shape))
    arrived = lax.all_to_all(copies, axis, split_axis=0, concat_axis=0, tiled=True)
    return arrived.reshape(-1, value.shape[-1])


def summed_on_arrival(value, axis):
    blocks = value.reshape(lax.axis_size(axis), -1, value.shape[-1])
    arrived = lax.all_to_all(blocks, axis, split_axis=0, concat_axis=0, tiled=True)
    return arrived.astype(jnp.float32).sum(axis=0)


def gelu_both(values):
    inner_arg = gelu_scale * (values + gelu_cubic * values * values * values)
    tanh_val = jnp.tanh(inner_arg)
    half = 0.5 * (1.0 + tanh_val)
    slope = half + 0.5 * values * (1.0 - tanh_val * tanh_val) * gelu_scale * (
        1.0 + 3.0 * gelu_cubic * values * values
    )
    return (values * half, slope)


def normalize(inputs):
    values = inputs.astype(jnp.float32)
    center = values - jnp.mean(values, axis=1, keepdims=True)
    inv_std = lax.rsqrt(jnp.mean(center * center, axis=1, keepdims=True) + layer_eps)
    return (center * inv_std, inv_std)


def contract_last(left, right):
    return lax.dot_general(
        left, right, (((1,), (1,)), ((), ())), preferred_element_type=jnp.float32
    )


def contract_first(left, right):
    return lax.dot_general(
        left, right, (((0,), (0,)), ((), ())), preferred_element_type=jnp.float32
    )


def times(left, right):
    return jnp.dot(left, right, preferred_element_type=jnp.float32)


def pick_fresh(mask_row):
    rows = mask_row.shape[0]
    fresh = (mask_row > 0).astype(jnp.float32)
    before = (jnp.arange(rows)[:, None] <= jnp.arange(rows)[None, :]).astype(jnp.float32)
    rank = jnp.sum(before * fresh[:, None], axis=0)
    wanted = jnp.arange(1, FRESH + 1).astype(jnp.float32)
    return jnp.where(rank[None, :] == wanted[:, None], fresh[None, :], 0.0)


def rows_at(picked, values):
    return times(picked.astype(jnp.bfloat16), values)


def body(
    video_tokens,
    cached_out,
    fresh_mask,
    timestep,
    up_weight,
    down_weight,
    router_in,
    router_bias,
    router_out,
    out_cotangent,
):
    second_section = lax.axis_index("pipe") == 1
    near = lax.axis_index("fsdp_1")
    along = lax.axis_index("fsdp_0")
    column_slot = lax.axis_index(FSDP)
    cached = cached_out[0, 0]
    w_up = up_weight[0]
    w_down = down_weight[0]
    r_in = router_in[0]
    r_out = router_out[0]
    features = cached.shape[1]
    hidden = r_in.shape[1]
    shard_cols = r_in.shape[0]
    near_count = lax.axis_size("fsdp_1")
    along_count = lax.axis_size("fsdp_0")
    group_rows = along_count * FRESH
    pair_cols = near_count * shard_cols
    bias_row = lax.dynamic_slice_in_dim(router_bias[0], timestep[0], 1)

    cached_before = lax.ppermute(cached, "pipe", [(0, 1)])
    picked = pick_fresh(fresh_mask[0, 0])
    live = jnp.sum(picked, axis=1, keepdims=True)

    def gate_of(router_pre):
        value, slope = gelu_both(router_pre)
        gate = jax.nn.sigmoid(jnp.sum(value * r_out[None, :], axis=1, keepdims=True))
        return (value, slope, gate)

    def columns_of(rows):
        return lax.dynamic_slice_in_dim(rows, along * pair_cols, pair_cols, 1)

    def first_part():
        rows_first = rows_at(picked, video_tokens[0])
        rows_cached = rows_at(picked, cached)
        scaled_first, _ = normalize(rows_first)
        gathered = from_everyone(scaled_first.astype(jnp.bfloat16), FSDP)
        act_first, _ = gelu_both(contract_last(gathered, w_up))
        terms = times(act_first.astype(jnp.bfloat16), w_down)
        columns = lax.dynamic_slice_in_dim(gathered, column_slot * shard_cols, shard_cols, 1)
        sums_first = summed_on_arrival(
            jnp.concatenate([terms, times(columns, r_in)], axis=1).astype(jnp.bfloat16), FSDP
        )
        by_near = gathered.reshape(along_count, near_count, FRESH, features)
        group_first = lax.dynamic_index_in_dim(by_near, near, 1, keepdims=False)
        columns_first = columns_of(group_first.reshape(group_rows, features))
        value_first, slope_first, gate_first = gate_of(sums_first[:, features:] + bias_row)
        change_first = rows_first + sums_first[:, :features] - rows_cached
        added_first = live * gate_first * change_first
        nothing = (
            jnp.zeros_like(w_up),
            jnp.zeros_like(w_down),
            jnp.zeros_like(r_in),
            jnp.zeros((group_rows, near_count * w_down.shape[0]), jnp.float32),
        )
        passing = jnp.concatenate([added_first, change_first, picked], axis=1)
        state = (value_first, slope_first, gate_first, rows_cached, columns_first)
        return (passing, state, rows_cached, nothing)

    def second_waits():
        swap = [(1, 3), (3, 1)]
        cot_rows = rows_at(picked, out_cotangent[0])
        group = from_everyone(cot_rows.astype(jnp.bfloat16), "fsdp_0")
        other_up = lax.ppermute(w_up, ("fsdp_1", "pipe"), swap)
        other_down = lax.ppermute(w_down, ("fsdp_1", "pipe"), swap)
        other_in = lax.ppermute(r_in, ("fsdp_1", "pipe"), swap)
        act_grad = jnp.concatenate(
            [contract_last(group, w_down), contract_last(group, other_down)], axis=1
        )
        row = jnp.zeros((FRESH, hidden), jnp.float32)
        state = (
            row,
            row,
            row[:, :1],
            rows_at(picked, cached),
            jnp.zeros((group_rows, pair_cols), jnp.bfloat16),
        )
        passing = jnp.zeros((FRESH, 2 * features + picked.shape[1]), jnp.float32)
        return (passing, state, cot_rows, (other_up, other_down, other_in, act_grad))

    passing, state, cot, others = lax.cond(second_section, second_waits, first_part)
    passed = lax.ppermute(passing, "pipe", [(0, 1)])

    def second_part():
        other_up, other_down, other_in, act_grad = others
        rows_cached = state[3]
        match = contract_last(picked, passed[:, 2 * features :])

        def at_match(values):
            return match[:, :1] * values[:1] + match[:, 1:] * values[1:]

        rows_second = rows_at(picked, cached_before) + at_match(passed[:, :features])
        rows_second = rows_second.astype(jnp.bfloat16).astype(jnp.float32)
        moved = at_match(passed[:, features : 2 * features])
        scaled, inv_std = normalize(rows_second)
        tangent = inv_std * (
            moved
            - jnp.mean(moved, axis=1, keepdims=True)
            - scaled * jnp.mean(moved * scaled, axis=1, keepdims=True)
        )
        both = jnp.concatenate([scaled, tangent], axis=1).astype(jnp.bfloat16)
        both = from_everyone(both, "fsdp_0")
        normed_group = both[:, :features]
        stacked = jnp.concatenate([normed_group, both[:, features:]])
        pre_both = jnp.concatenate(
            [contract_last(stacked, w_up), contract_last(stacked, other_up)], axis=1
        )
        act, act_slope = gelu_both(pre_both[:group_rows])
        act = act.astype(jnp.bfloat16)
        own_units = w_down.shape[0]
        terms = times(act[:, :own_units], w_down) + times(act[:, own_units:], other_down)
        slope_terms = jnp.sum(act_grad * act_slope * pre_both[group_rows:], axis=1, keepdims=True)
        in_pair = jnp.where(
            near == 0, jnp.concatenate([r_in, other_in]), jnp.concatenate([other_in, r_in])
        )
        columns = columns_of(stacked)
        routed = times(columns, in_pair)
        sums = summed_on_arrival(
            jnp.concatenate(
                [
                    terms,
                    routed[:group_rows],
                    routed[group_rows:],
                    jnp.broadcast_to(slope_terms, (group_rows, 128)),
                ],
                axis=1,
            ).astype(jnp.bfloat16),
            "fsdp_0",
        )
        value, slope, gate = gate_of(sums[:, features : features + hidden] + bias_row)
        change = rows_second + sums[:, :features] - rows_cached
        gate_grad = live * jnp.sum(cot * change, axis=1, keepdims=True)
        logit_grad = gate_grad * gate * (1.0 - gate)
        routed_tangent = sums[:, features + hidden : features + 2 * hidden]
        input_grad = live * gate * (
            jnp.sum(cot * moved, axis=1, keepdims=True) + sums[:, features + 2 * hidden :][:, :1]
        ) + logit_grad * jnp.sum(r_out[None, :] * slope * routed_tangent, axis=1, keepdims=True)
        returning = jnp.sum(match * input_grad, axis=0)
        return (
            returning,
            rows_cached + live * gate * change,
            value,
            slope,
            logit_grad,
            columns[:group_rows],
        )

    def first_waits():
        value_first, slope_first, gate_first, rows_cached, columns_first = state
        return (
            jnp.zeros((FRESH,), jnp.float32),
            rows_cached + passing[:, :features],
            value_first,
            slope_first,
            gate_first * (1.0 - gate_first),
            columns_first,
        )

    returning, new_rows, value, slope, logit_grad, pair_columns = lax.cond(
        second_section, second_part, first_waits
    )

    returned = lax.ppermute(returning, "pipe", [(1, 0)])[:, None]
    logit_grad = jnp.where(second_section, logit_grad, live * returned * logit_grad)
    late = jnp.concatenate([logit_grad * r_out[None, :] * slope, logit_grad * value], axis=1)
    late = from_everyone(late.astype(jnp.bfloat16), "fsdp_0")
    in_grad = contract_first(pair_columns, late[:, :hidden])
    totals = jnp.sum(late.astype(jnp.float32), axis=0).reshape(2, hidden)
    step_row = jnp.broadcast_to(timestep[0].astype(jnp.float32), (1, hidden))
    dp_count = lax.axis_size("dp")
    extra = jnp.concatenate([totals, step_row])
    message = jnp.concatenate(
        [
            in_grad.reshape(near_count, shard_cols, hidden),
            jnp.broadcast_to(extra, (near_count, *extra.shape)),
        ],
        axis=1,
    ).astype(jnp.bfloat16)
    message = jnp.broadcast_to(message[:, None], (near_count, dp_count, *message.shape[1:]))
    arrived = lax.all_to_all(
        message.reshape(-1, *message.shape[2:]), PLANE, split_axis=0, concat_axis=0, tiled=True
    ).astype(jnp.float32)
    summed_in = jnp.sum(arrived[:, :shard_cols], axis=0)
    bias_parts = arrived[:, shard_cols]
    summed_out = jnp.sum(arrived[:, shard_cols + 1], axis=0)
    steps = jnp.arange(router_bias.shape[1]).astype(jnp.float32)
    is_step = steps[:, None] == arrived[:, shard_cols + 2, 0][None, :]
    summed_bias = jnp.sum(jnp.where(is_step[:, :, None], bias_parts[None], 0.0), axis=1)

    new_rows = new_rows.astype(jnp.bfloat16)
    blended = cached
    for row in range(FRESH):
        blended = jnp.where(picked[row][:, None] > 0, new_rows[row][None, :], blended)
    return (blended[None, None], summed_in[None], summed_bias[None], summed_out[None])


def solution(mesh):
    torus = Mesh(
        mesh.devices.reshape(16, 2, mesh.shape["pipe"], mesh.shape["dp"]),
        ("fsdp_0", "fsdp_1", "pipe", "dp"),
    )
    return jax.shard_map(
        body,
        mesh=torus,
        in_specs=(
            P("dp", FSDP, None),
            P("pipe", "dp", FSDP, None),
            P("pipe", "dp", FSDP),
            P("dp"),
            P("pipe", FSDP, None),
            P("pipe", FSDP, None),
            P("pipe", FSDP, None),
            P("pipe", None, None),
            P("pipe", None),
            P("dp", FSDP, None),
        ),
        out_specs=(
            P("pipe", "dp", FSDP, None),
            P("pipe", FSDP, None),
            P("pipe", None, None),
            P("pipe", None),
        ),
        check_vma=False,
    )
```

```python
import jax
import jax.numpy as jnp
from jax import lax
from jax.experimental import pallas as pl
from jax.sharding import Mesh
from jax.sharding import PartitionSpec as P

FRESH = 2
FSDP = ("fsdp_0", "fsdp_1")
PLANE = ("fsdp_1", "dp")


layer_eps = 1e-06
gelu_scale = 0.7978845608028654
gelu_cubic = 0.044715


def from_everyone(value, axis):
    copies = jnp.broadcast_to(value, (lax.axis_size(axis), *value.shape))
    arrived = lax.all_to_all(copies, axis, split_axis=0, concat_axis=0, tiled=True)
    return arrived.reshape(-1, value.shape[-1])


def summed_on_arrival(value, axis):
    blocks = value.reshape(lax.axis_size(axis), -1, value.shape[-1])
    arrived = lax.all_to_all(blocks, axis, split_axis=0, concat_axis=0, tiled=True)
    return arrived.astype(jnp.float32).sum(axis=0)


def gelu_both(values):
    inner_arg = gelu_scale * (values + gelu_cubic * values * values * values)
    tanh_val = jnp.tanh(inner_arg)
    half = 0.5 * (1.0 + tanh_val)
    slope = half + 0.5 * values * (1.0 - tanh_val * tanh_val) * gelu_scale * (
        1.0 + 3.0 * gelu_cubic * values * values
    )
    return (values * half, slope)


def normalize(inputs):
    values = inputs.astype(jnp.float32)
    center = values - jnp.mean(values, axis=1, keepdims=True)
    inv_std = lax.rsqrt(jnp.mean(center * center, axis=1, keepdims=True) + layer_eps)
    return (center * inv_std, inv_std)


def contract_last(left, right):
    return lax.dot_general(
        left, right, (((1,), (1,)), ((), ())), preferred_element_type=jnp.float32
    )


def contract_first(left, right):
    return lax.dot_general(
        left, right, (((0,), (0,)), ((), ())), preferred_element_type=jnp.float32
    )


def times(left, right):
    return jnp.dot(left, right, preferred_element_type=jnp.float32)


def unset(*arrays):
    return pl.pallas_call(
        lambda *refs: None,
        out_shape=[jax.ShapeDtypeStruct(shape, dtype) for shape, dtype in arrays],
        out_specs=[pl.BlockSpec(memory_space=pl.ANY)] * len(arrays),
    )()


def pick_fresh(mask_row):
    rows = mask_row.shape[0]
    fresh = (mask_row > 0).astype(jnp.float32)
    before = (jnp.arange(rows)[:, None] <= jnp.arange(rows)[None, :]).astype(jnp.float32)
    rank = jnp.sum(before * fresh[:, None], axis=0)
    wanted = jnp.arange(1, FRESH + 1).astype(jnp.float32)
    return jnp.where(rank[None, :] == wanted[:, None], fresh[None, :], 0.0)


def rows_at(picked, values):
    return times(picked.astype(jnp.bfloat16), values)


def body(
    video_tokens,
    cached_out,
    fresh_mask,
    timestep,
    up_weight,
    down_weight,
    router_in,
    router_bias,
    router_out,
    out_cotangent,
):
    second_section = lax.axis_index("pipe") == 1
    near = lax.axis_index("fsdp_1")
    along = lax.axis_index("fsdp_0")
    column_slot = lax.axis_index(FSDP)
    cached = cached_out[0, 0]
    w_up = up_weight[0]
    w_down = down_weight[0]
    r_in = router_in[0]
    r_out = router_out[0]
    features = cached.shape[1]
    hidden = r_in.shape[1]
    shard_cols = r_in.shape[0]
    near_count = lax.axis_size("fsdp_1")
    along_count = lax.axis_size("fsdp_0")
    group_rows = along_count * FRESH
    dp_count = lax.axis_size("dp")
    plane_count = near_count * dp_count
    pair_cols = near_count * shard_cols
    bias_row = lax.dynamic_slice_in_dim(router_bias[0], timestep[0], 1)

    cached_before = lax.ppermute(cached, "pipe", [(0, 1)])
    picked = pick_fresh(fresh_mask[0, 0])
    live = jnp.sum(picked, axis=1, keepdims=True)

    def gate_of(router_pre):
        value, slope = gelu_both(router_pre)
        gate = jax.nn.sigmoid(jnp.sum(value * r_out[None, :], axis=1, keepdims=True))
        return (value, slope, gate)

    def columns_of(rows):
        return lax.dynamic_slice_in_dim(rows, along * pair_cols, pair_cols, 1)

    def from_next(value, section):
        place = lambda x_hi, dp: (x_hi * 2 + section) * dp_count + dp
        route = [
            (place(x_hi, dp), place(1 - x_hi, dp ^ (dp_count // 2)))
            for x_hi in range(near_count)
            for dp in range(dp_count)
        ]
        return lax.ppermute(value, ("fsdp_1", "pipe", "dp"), route)

    def first_part():
        rows_first = rows_at(picked, video_tokens[0])
        rows_cached = rows_at(picked, cached)
        scaled_first, _ = normalize(rows_first)
        own = from_everyone(scaled_first.astype(jnp.bfloat16), "fsdp_0")
        other = from_next(own, 0)

        def partial_sums(rows):
            act_first, _ = gelu_both(contract_last(rows, w_up))
            terms = times(act_first.astype(jnp.bfloat16), w_down)
            columns = lax.dynamic_slice_in_dim(rows, column_slot * shard_cols, shard_cols, 1)
            return jnp.concatenate([terms, times(columns, r_in)], axis=1)

        returned = from_next(partial_sums(other).astype(jnp.bfloat16), 0)
        sums_first = (partial_sums(own) + returned.astype(jnp.float32)).astype(jnp.bfloat16)
        sums_first = summed_on_arrival(sums_first, "fsdp_0")
        columns_first = columns_of(own)
        value_first, slope_first, gate_first = gate_of(sums_first[:, features:] + bias_row)
        change_first = rows_first + sums_first[:, :features] - rows_cached
        added_first = live * gate_first * change_first
        nothing = unset(
            (w_up.shape, w_up.dtype),
            (w_down.shape, w_down.dtype),
            (r_in.shape, r_in.dtype),
            ((group_rows, near_count * w_down.shape[0]), jnp.float32),
        )
        passing = jnp.concatenate([added_first, change_first, picked], axis=1)
        state = (value_first, slope_first, gate_first, rows_cached, columns_first)
        return (passing, state, rows_cached, tuple(nothing))

    def second_waits():
        cot_rows = rows_at(picked, out_cotangent[0])
        group = from_everyone(cot_rows.astype(jnp.bfloat16), "fsdp_0")
        other_up = from_next(w_up, 1)
        other_down = from_next(w_down, 1)
        other_in = from_next(r_in, 1)
        act_grad = jnp.concatenate(
            [contract_last(group, w_down), contract_last(group, other_down)], axis=1
        )
        row = jnp.zeros((FRESH, hidden), jnp.float32)
        (columns,) = unset(((group_rows, pair_cols), jnp.bfloat16))
        state = (row, row, row[:, :1], rows_at(picked, cached), columns)
        passing = jnp.zeros((FRESH, 2 * features + picked.shape[1]), jnp.float32)
        return (passing, state, cot_rows, (other_up, other_down, other_in, act_grad))

    passing, state, cot, others = lax.cond(second_section, second_waits, first_part)
    passed = lax.ppermute(passing, "pipe", [(0, 1)])

    def second_part():
        other_up, other_down, other_in, act_grad = others
        rows_cached = state[3]
        match = contract_last(picked, passed[:, 2 * features :])

        def at_match(values):
            return match[:, :1] * values[:1] + match[:, 1:] * values[1:]

        rows_second = rows_at(picked, cached_before) + at_match(passed[:, :features])
        rows_second = rows_second.astype(jnp.bfloat16).astype(jnp.float32)
        moved = at_match(passed[:, features : 2 * features])
        scaled, inv_std = normalize(rows_second)
        tangent = inv_std * (
            moved
            - jnp.mean(moved, axis=1, keepdims=True)
            - scaled * jnp.mean(moved * scaled, axis=1, keepdims=True)
        )
        both = jnp.concatenate([scaled, tangent], axis=1).astype(jnp.bfloat16)
        both = from_everyone(both, "fsdp_0")
        normed_group = both[:, :features]
        stacked = jnp.concatenate([normed_group, both[:, features:]])
        pre_both = jnp.concatenate(
            [contract_last(stacked, w_up), contract_last(stacked, other_up)], axis=1
        )
        act, act_slope = gelu_both(pre_both[:group_rows])
        act = act.astype(jnp.bfloat16)
        own_units = w_down.shape[0]
        terms = times(act[:, :own_units], w_down) + times(act[:, own_units:], other_down)
        slope_terms = jnp.sum(act_grad * act_slope * pre_both[group_rows:], axis=1, keepdims=True)
        in_pair = jnp.where(
            near == 0, jnp.concatenate([r_in, other_in]), jnp.concatenate([other_in, r_in])
        )
        columns = columns_of(stacked)
        routed = times(columns, in_pair)
        sums = jnp.concatenate(
            [
                terms,
                routed[:group_rows],
                routed[group_rows:],
                jnp.broadcast_to(slope_terms, (group_rows, 128)),
            ],
            axis=1,
        ).astype(jnp.bfloat16)
        sums = summed_on_arrival(sums, "fsdp_0")
        value, slope, gate = gate_of(sums[:, features : features + hidden] + bias_row)
        change = rows_second + sums[:, :features] - rows_cached
        gate_grad = live * jnp.sum(cot * change, axis=1, keepdims=True)
        logit_grad = gate_grad * gate * (1.0 - gate)
        routed_tangent = sums[:, features + hidden : features + 2 * hidden]
        input_grad = live * gate * (
            jnp.sum(cot * moved, axis=1, keepdims=True) + sums[:, features + 2 * hidden :][:, :1]
        ) + logit_grad * jnp.sum(r_out[None, :] * slope * routed_tangent, axis=1, keepdims=True)
        returning = jnp.sum(match * input_grad, axis=0)
        return (
            returning,
            rows_cached + live * gate * change,
            value,
            slope,
            logit_grad,
            columns[:group_rows],
        )

    def first_waits():
        value_first, slope_first, gate_first, rows_cached, columns_first = state
        return (
            jnp.zeros((FRESH,), jnp.float32),
            rows_cached + passing[:, :features],
            value_first,
            slope_first,
            gate_first * (1.0 - gate_first),
            columns_first,
        )

    returning, new_rows, value, slope, logit_grad, pair_columns = lax.cond(
        second_section, second_part, first_waits
    )

    returned = lax.ppermute(returning, "pipe", [(1, 0)])[:, None]
    logit_grad = jnp.where(second_section, logit_grad, live * returned * logit_grad)
    late = jnp.concatenate([logit_grad * r_out[None, :] * slope, logit_grad * value], axis=1)
    late = from_everyone(late.astype(jnp.bfloat16), "fsdp_0")
    out_row = jnp.sum(late[:, hidden:].astype(jnp.float32), axis=0, keepdims=True)
    step_row = jnp.broadcast_to(timestep[0].astype(jnp.float32), (1, hidden))
    hidden_part = jnp.concatenate(
        [late[:, :hidden], out_row.astype(jnp.bfloat16), step_row.astype(jnp.bfloat16)]
    )
    shards = jnp.moveaxis(pair_columns.reshape(group_rows, near_count, shard_cols), 1, 0)
    shards = jnp.pad(shards, ((0, 0), (0, 2), (0, 128 - shard_cols)))
    message = jnp.concatenate(
        [jnp.broadcast_to(hidden_part, (near_count, *hidden_part.shape)), shards], axis=2
    )
    message = jnp.broadcast_to(message[:, None], (near_count, dp_count, *message.shape[1:]))
    arrived = lax.all_to_all(
        message.reshape(plane_count, *message.shape[2:]), PLANE, 0, 0, tiled=True
    )
    plane_rows = arrived[:, :group_rows].reshape(plane_count * group_rows, -1)
    hidden_rows = plane_rows[:, :hidden]
    summed_in = contract_first(plane_rows[:, hidden : hidden + shard_cols], hidden_rows)
    steps = jnp.arange(router_bias.shape[1]).astype(jnp.bfloat16)
    is_step = (steps[:, None] == arrived[:, group_rows + 1, 0][None, :]).astype(jnp.bfloat16)
    summed_bias = times(jnp.repeat(is_step, group_rows, axis=1), hidden_rows)
    summed_out = jnp.sum(arrived[:, group_rows, :hidden].astype(jnp.float32), axis=0)

    new_rows = new_rows.astype(jnp.bfloat16)
    blended = cached
    for row in range(FRESH):
        blended = jnp.where(picked[row][:, None] > 0, new_rows[row][None, :], blended)
    return (blended[None, None], summed_in[None], summed_bias[None], summed_out[None])


def solution(mesh):
    torus = Mesh(
        mesh.devices.reshape(16, 2, mesh.shape["pipe"], mesh.shape["dp"]),
        ("fsdp_0", "fsdp_1", "pipe", "dp"),
    )
    return jax.shard_map(
        body,
        mesh=torus,
        in_specs=(
            P("dp", FSDP, None),
            P("pipe", "dp", FSDP, None),
            P("pipe", "dp", FSDP),
            P("dp"),
            P("pipe", FSDP, None),
            P("pipe", FSDP, None),
            P("pipe", FSDP, None),
            P("pipe", None, None),
            P("pipe", None),
            P("dp", FSDP, None),
        ),
        out_specs=(
            P("pipe", "dp", FSDP, None),
            P("pipe", FSDP, None),
            P("pipe", None, None),
            P("pipe", None),
        ),
        check_vma=False,
    )
```

```python
import jax
import jax.numpy as jnp
from jax import lax
from jax.experimental import pallas as pl
from jax.sharding import Mesh
from jax.sharding import PartitionSpec as P


FRESH = 2
FSDP = ("fsdp_0", "fsdp_1")
PLANE = ("fsdp_1", "dp")


layer_eps = 1e-06
gelu_scale = 0.7978845608028654
gelu_cubic = 0.044715


def from_everyone(value, axis):
    copies = jnp.broadcast_to(value, (lax.axis_size(axis), *value.shape))
    arrived = lax.all_to_all(copies, axis, split_axis=0, concat_axis=0, tiled=True)
    return arrived.reshape(-1, value.shape[-1])


def summed_on_arrival(value, axis):
    blocks = value.reshape(lax.axis_size(axis), -1, value.shape[-1])
    arrived = lax.all_to_all(blocks, axis, split_axis=0, concat_axis=0, tiled=True)
    return arrived.astype(jnp.float32).sum(axis=0)


def gelu_both(values):
    inner_arg = gelu_scale * (values + gelu_cubic * values * values * values)
    tanh_val = jnp.tanh(inner_arg)
    half = 0.5 * (1.0 + tanh_val)
    slope = half + 0.5 * values * (1.0 - tanh_val * tanh_val) * gelu_scale * (
        1.0 + 3.0 * gelu_cubic * values * values
    )
    return (values * half, slope)


def normalize(inputs):
    values = inputs.astype(jnp.float32)
    center = values - jnp.mean(values, axis=1, keepdims=True)
    inv_std = lax.rsqrt(jnp.mean(center * center, axis=1, keepdims=True) + layer_eps)
    return (center * inv_std, inv_std)


def contract_last(left, right):
    return lax.dot_general(
        left, right, (((1,), (1,)), ((), ())), preferred_element_type=jnp.float32
    )


def contract_first(left, right):
    return lax.dot_general(
        left, right, (((0,), (0,)), ((), ())), preferred_element_type=jnp.float32
    )


def times(left, right):
    return jnp.dot(left, right, preferred_element_type=jnp.float32)


def unset(*arrays):
    return pl.pallas_call(
        lambda *refs: None,
        out_shape=[jax.ShapeDtypeStruct(shape, dtype) for shape, dtype in arrays],
        out_specs=[pl.BlockSpec(memory_space=pl.ANY)] * len(arrays),
    )()


def pick_fresh(mask_row):
    rows = mask_row.shape[0]
    fresh = (mask_row > 0).astype(jnp.float32)
    before = (jnp.arange(rows)[:, None] <= jnp.arange(rows)[None, :]).astype(jnp.float32)
    rank = jnp.sum(before * fresh[:, None], axis=0)
    wanted = jnp.arange(1, FRESH + 1).astype(jnp.float32)
    return jnp.where(rank[None, :] == wanted[:, None], fresh[None, :], 0.0)


def rows_at(picked, values):
    return times(picked.astype(jnp.bfloat16), values)


def body(
    video_tokens,
    cached_out,
    fresh_mask,
    timestep,
    up_weight,
    down_weight,
    router_in,
    router_bias,
    router_out,
    out_cotangent,
):
    second_section = lax.axis_index("pipe") == 1
    near = lax.axis_index("fsdp_1")
    along = lax.axis_index("fsdp_0")
    cached = cached_out[0, 0]
    w_up = up_weight[0]
    w_down = down_weight[0]
    r_in = router_in[0]
    r_out = router_out[0]
    features = cached.shape[1]
    hidden = r_in.shape[1]
    shard_cols = r_in.shape[0]
    near_count = lax.axis_size("fsdp_1")
    along_count = lax.axis_size("fsdp_0")
    group_rows = along_count * FRESH
    dp_count = lax.axis_size("dp")
    plane_count = near_count * dp_count
    pair_cols = near_count * shard_cols
    bias_row = lax.dynamic_slice_in_dim(router_bias[0], timestep[0], 1)

    cached_before = lax.ppermute(cached, "pipe", [(0, 1)])
    picked = pick_fresh(fresh_mask[0, 0])
    live = jnp.sum(picked, axis=1, keepdims=True)

    def gate_of(router_pre):
        value, slope = gelu_both(router_pre)
        gate = jax.nn.sigmoid(jnp.sum(value * r_out[None, :], axis=1, keepdims=True))
        return (value, slope, gate)

    def columns_of(rows):
        return lax.dynamic_slice_in_dim(rows, along * pair_cols, pair_cols, 1)

    def from_next(value, section):
        place = lambda x_hi, dp: (x_hi * 2 + section) * dp_count + dp
        route = [
            (place(x_hi, dp), place(1 - x_hi, dp ^ (dp_count // 2)))
            for x_hi in range(near_count)
            for dp in range(dp_count)
        ]
        return lax.ppermute(value, ("fsdp_1", "pipe", "dp"), route)

    def other_shards(section):
        swapped = []
        for value in (w_up, w_down, r_in):
            swapped.append(from_next(value, section))
        return tuple(swapped)

    def paired_in(other_in):
        return jnp.where(
            near == 0, jnp.concatenate([r_in, other_in]), jnp.concatenate([other_in, r_in])
        )

    def up_both(rows, other_up):
        return jnp.concatenate([contract_last(rows, w_up), contract_last(rows, other_up)], axis=1)

    def down_both(act, other_down):
        act = act.astype(jnp.bfloat16)
        own_units = w_down.shape[0]
        return times(act[:, :own_units], w_down) + times(act[:, own_units:], other_down)

    def first_part():
        other_up, other_down, other_in = other_shards(0)
        rows_first = rows_at(picked, video_tokens[0])
        rows_cached = rows_at(picked, cached)
        scaled_first, _ = normalize(rows_first)
        own = from_everyone(scaled_first.astype(jnp.bfloat16), "fsdp_0")
        act_first, _ = gelu_both(up_both(own, other_up))
        columns_first = columns_of(own)
        routed = times(columns_first, paired_in(other_in))
        sums_first = jnp.concatenate([down_both(act_first, other_down), routed], axis=1)
        sums_first = summed_on_arrival(sums_first.astype(jnp.bfloat16), "fsdp_0")
        value_first, slope_first, gate_first = gate_of(sums_first[:, features:] + bias_row)
        change_first = rows_first + sums_first[:, :features] - rows_cached
        added_first = live * gate_first * change_first
        nothing = unset(
            (w_up.shape, w_up.dtype),
            (w_down.shape, w_down.dtype),
            (r_in.shape, r_in.dtype),
            ((group_rows, near_count * w_down.shape[0]), jnp.float32),
        )
        passing = jnp.concatenate([added_first, change_first, picked], axis=1)
        state = (value_first, slope_first, gate_first, rows_cached, columns_first)
        return (passing, state, rows_cached, tuple(nothing))

    def second_waits():
        cot_rows = rows_at(picked, out_cotangent[0])
        group = from_everyone(cot_rows.astype(jnp.bfloat16), "fsdp_0")
        other_up, other_down, other_in = other_shards(1)
        act_grad = jnp.concatenate(
            [contract_last(group, w_down), contract_last(group, other_down)], axis=1
        )
        row = jnp.zeros((FRESH, hidden), jnp.float32)
        (columns,) = unset(((group_rows, pair_cols), jnp.bfloat16))
        state = (row, row, row[:, :1], rows_at(picked, cached), columns)
        passing = jnp.zeros((FRESH, 2 * features + picked.shape[1]), jnp.float32)
        return (passing, state, cot_rows, (other_up, other_down, other_in, act_grad))

    passing, state, cot, others = lax.cond(second_section, second_waits, first_part)
    passed = lax.ppermute(passing, "pipe", [(0, 1)])
    cached_asked = rows_at(picked, cached_before)

    def second_part():
        other_up, other_down, other_in, act_grad = others
        rows_cached = state[3]
        match = contract_last(picked, passed[:, 2 * features :])

        def at_match(values):
            return match[:, :1] * values[:1] + match[:, 1:] * values[1:]

        rows_second = cached_asked + at_match(passed[:, :features])
        rows_second = rows_second.astype(jnp.bfloat16).astype(jnp.float32)
        moved = at_match(passed[:, features : 2 * features])
        scaled, inv_std = normalize(rows_second)
        tangent = inv_std * (
            moved
            - jnp.mean(moved, axis=1, keepdims=True)
            - scaled * jnp.mean(moved * scaled, axis=1, keepdims=True)
        )
        both = jnp.concatenate([scaled, tangent], axis=1).astype(jnp.bfloat16)
        both = from_everyone(both, "fsdp_0")
        normed_group = both[:, :features]
        stacked = jnp.concatenate([normed_group, both[:, features:]])
        pre_both = up_both(stacked, other_up)
        act, act_slope = gelu_both(pre_both[:group_rows])
        terms = down_both(act, other_down)
        slope_terms = jnp.sum(act_grad * act_slope * pre_both[group_rows:], axis=1, keepdims=True)
        columns = columns_of(stacked)
        routed = times(columns, paired_in(other_in))
        sums = jnp.concatenate(
            [
                terms,
                routed[:group_rows],
                routed[group_rows:],
                jnp.broadcast_to(slope_terms, (group_rows, 128)),
            ],
            axis=1,
        ).astype(jnp.bfloat16)
        sums = summed_on_arrival(sums, "fsdp_0")
        value, slope, gate = gate_of(sums[:, features : features + hidden] + bias_row)
        change = rows_second + sums[:, :features] - rows_cached
        gate_grad = live * jnp.sum(cot * change, axis=1, keepdims=True)
        logit_grad = gate_grad * gate * (1.0 - gate)
        routed_tangent = sums[:, features + hidden : features + 2 * hidden]
        input_grad = live * gate * (
            jnp.sum(cot * moved, axis=1, keepdims=True) + sums[:, features + 2 * hidden :][:, :1]
        ) + logit_grad * jnp.sum(r_out[None, :] * slope * routed_tangent, axis=1, keepdims=True)
        returning = jnp.sum(match * input_grad, axis=0)
        return (
            returning,
            rows_cached + live * gate * change,
            value,
            slope,
            logit_grad,
            columns[:group_rows],
        )

    def first_waits():
        value_first, slope_first, gate_first, rows_cached, columns_first = state
        return (
            jnp.zeros((FRESH,), jnp.float32),
            rows_cached + passing[:, :features],
            value_first,
            slope_first,
            gate_first * (1.0 - gate_first),
            columns_first,
        )

    returning, new_rows, value, slope, logit_grad, pair_columns = lax.cond(
        second_section, second_part, first_waits
    )

    returned = lax.ppermute(returning, "pipe", [(1, 0)])[:, None]
    logit_grad = jnp.where(second_section, logit_grad, live * returned * logit_grad)
    late = jnp.concatenate([logit_grad * r_out[None, :] * slope, logit_grad * value], axis=1)
    late = from_everyone(late.astype(jnp.bfloat16), "fsdp_0")
    out_row = jnp.sum(late[:, hidden:].astype(jnp.float32), axis=0, keepdims=True)
    step_row = jnp.broadcast_to(timestep[0].astype(jnp.float32), (1, hidden))
    hidden_part = jnp.concatenate(
        [late[:, :hidden], out_row.astype(jnp.bfloat16), step_row.astype(jnp.bfloat16)]
    )
    shards = jnp.moveaxis(pair_columns.reshape(group_rows, near_count, shard_cols), 1, 0)
    shards = jnp.pad(shards, ((0, 0), (0, 2), (0, 128 - shard_cols)))
    message = jnp.concatenate(
        [jnp.broadcast_to(hidden_part, (near_count, *hidden_part.shape)), shards], axis=2
    )
    message = jnp.broadcast_to(message[:, None], (near_count, dp_count, *message.shape[1:]))
    arrived = lax.all_to_all(
        message.reshape(plane_count, *message.shape[2:]), PLANE, 0, 0, tiled=True
    )
    plane_rows = arrived[:, :group_rows].reshape(plane_count * group_rows, -1)
    hidden_rows = plane_rows[:, :hidden]
    summed_in = contract_first(plane_rows[:, hidden : hidden + shard_cols], hidden_rows)
    steps = jnp.arange(router_bias.shape[1]).astype(jnp.bfloat16)
    is_step = (steps[:, None] == arrived[:, group_rows + 1, 0][None, :]).astype(jnp.bfloat16)
    summed_bias = times(jnp.repeat(is_step, group_rows, axis=1), hidden_rows)
    summed_out = jnp.sum(arrived[:, group_rows, :hidden].astype(jnp.float32), axis=0)

    new_rows = new_rows.astype(jnp.bfloat16)
    blended = cached
    for row in range(FRESH):
        blended = jnp.where(picked[row][:, None] > 0, new_rows[row][None, :], blended)
    return (blended[None, None], summed_in[None], summed_bias[None], summed_out[None])


def solution(mesh):
    torus = Mesh(
        mesh.devices.reshape(16, 2, mesh.shape["pipe"], mesh.shape["dp"]),
        ("fsdp_0", "fsdp_1", "pipe", "dp"),
    )
    return jax.shard_map(
        body,
        mesh=torus,
        in_specs=(
            P("dp", FSDP, None),
            P("pipe", "dp", FSDP, None),
            P("pipe", "dp", FSDP),
            P("dp"),
            P("pipe", FSDP, None),
            P("pipe", FSDP, None),
            P("pipe", FSDP, None),
            P("pipe", None, None),
            P("pipe", None),
            P("dp", FSDP, None),
        ),
        out_specs=(
            P("pipe", "dp", FSDP, None),
            P("pipe", FSDP, None),
            P("pipe", None, None),
            P("pipe", None),
        ),
        check_vma=False,
    )
```

```python
import jax
import jax.numpy as jnp
from jax import lax
from jax.experimental import pallas as pl
from jax.sharding import Mesh
from jax.sharding import PartitionSpec as P


FRESH = 2
FSDP = ("fsdp_0", "fsdp_1")
PLANE = ("fsdp_1", "dp")


layer_eps = 1e-06
gelu_scale = 0.7978845608028654
gelu_cubic = 0.044715


def from_everyone(value, axis):
    copies = jnp.broadcast_to(value, (lax.axis_size(axis), *value.shape))
    arrived = lax.all_to_all(copies, axis, split_axis=0, concat_axis=0, tiled=True)
    return arrived.reshape(-1, value.shape[-1])


def summed_on_arrival(value, axis):
    blocks = value.reshape(lax.axis_size(axis), -1, value.shape[-1])
    arrived = lax.all_to_all(blocks, axis, split_axis=0, concat_axis=0, tiled=True)
    return arrived.astype(jnp.float32).sum(axis=0)


def gelu_both(values):
    inner_arg = gelu_scale * (values + gelu_cubic * values * values * values)
    tanh_val = jnp.tanh(inner_arg)
    half = 0.5 * (1.0 + tanh_val)
    slope = half + 0.5 * values * (1.0 - tanh_val * tanh_val) * gelu_scale * (
        1.0 + 3.0 * gelu_cubic * values * values
    )
    return (values * half, slope)


def normalize(inputs):
    values = inputs.astype(jnp.float32)
    center = values - jnp.mean(values, axis=1, keepdims=True)
    inv_std = lax.rsqrt(jnp.mean(center * center, axis=1, keepdims=True) + layer_eps)
    return (center * inv_std, inv_std)


def contract_last(left, right):
    return lax.dot_general(
        left, right, (((1,), (1,)), ((), ())), preferred_element_type=jnp.float32
    )


def contract_first(left, right):
    return lax.dot_general(
        left, right, (((0,), (0,)), ((), ())), preferred_element_type=jnp.float32
    )


def times(left, right):
    return jnp.dot(left, right, preferred_element_type=jnp.float32)


def two_parts(values):
    upper = lax.reduce_precision(values, exponent_bits=8, mantissa_bits=7)
    return [upper, values - upper]


def unset(*arrays):
    return pl.pallas_call(
        lambda *refs: None,
        out_shape=[jax.ShapeDtypeStruct(shape, dtype) for shape, dtype in arrays],
        out_specs=[pl.BlockSpec(memory_space=pl.ANY)] * len(arrays),
    )()


def pick_fresh(mask_row):
    rows = mask_row.shape[0]
    fresh = (mask_row > 0).astype(jnp.float32)
    before = (jnp.arange(rows)[:, None] <= jnp.arange(rows)[None, :]).astype(jnp.float32)
    rank = jnp.sum(before * fresh[:, None], axis=0)
    wanted = jnp.arange(1, FRESH + 1).astype(jnp.float32)
    return jnp.where(rank[None, :] == wanted[:, None], fresh[None, :], 0.0)


def rows_at(picked, values):
    return times(picked.astype(jnp.bfloat16), values)


def body(
    video_tokens,
    cached_out,
    fresh_mask,
    timestep,
    up_weight,
    down_weight,
    router_in,
    router_bias,
    router_out,
    out_cotangent,
):
    second_section = lax.axis_index("pipe") == 1
    near = lax.axis_index("fsdp_1")
    along = lax.axis_index("fsdp_0")
    cached = cached_out[0, 0]
    w_up = up_weight[0]
    w_down = down_weight[0]
    r_in = router_in[0]
    r_out = router_out[0]
    features = cached.shape[1]
    hidden = r_in.shape[1]
    shard_cols = r_in.shape[0]
    near_count = lax.axis_size("fsdp_1")
    along_count = lax.axis_size("fsdp_0")
    group_rows = along_count * FRESH
    dp_count = lax.axis_size("dp")
    plane_count = near_count * dp_count
    pair_cols = near_count * shard_cols
    bias_row = lax.dynamic_slice_in_dim(router_bias[0], timestep[0], 1)

    cached_before = lax.ppermute(cached, "pipe", [(0, 1)])
    picked = pick_fresh(fresh_mask[0, 0])
    live = jnp.sum(picked, axis=1, keepdims=True)

    def gate_of(router_pre):
        value, slope = gelu_both(router_pre)
        gate = jax.nn.sigmoid(jnp.sum(value * r_out[None, :], axis=1, keepdims=True))
        return (value, slope, gate)

    def columns_of(rows):
        return lax.dynamic_slice_in_dim(rows, along * pair_cols, pair_cols, 1)

    def from_next(value, section):
        place = lambda x_hi, dp: (x_hi * 2 + section) * dp_count + dp
        route = [
            (place(x_hi, dp), place(1 - x_hi, dp ^ (dp_count // 2)))
            for x_hi in range(near_count)
            for dp in range(dp_count)
        ]
        return lax.ppermute(value, ("fsdp_1", "pipe", "dp"), route)

    def halves_from_next(value):
        half = value.shape[0] // 2
        far = lax.axis_index("dp") // (dp_count // 2)
        wanted = lax.dynamic_slice_in_dim(value, (1 - far) * half, half)
        got = from_next(wanted, 1)
        route = [(dp_count + dp, dp_count + (dp ^ (dp_count // 2))) for dp in range(dp_count)]
        shared = lax.ppermute(got, ("pipe", "dp"), route)
        return jnp.concatenate([got, shared])

    def other_shards(section):
        swapped = []
        for value in (w_up, w_down, r_in):
            swapped.append(from_next(value, section))
        return tuple(swapped)

    def paired_in(other_in):
        return jnp.where(
            near == 0, jnp.concatenate([r_in, other_in]), jnp.concatenate([other_in, r_in])
        )

    def up_both(rows, other_up):
        return jnp.concatenate([contract_last(rows, w_up), contract_last(rows, other_up)], axis=1)

    def down_both(act, other_down):
        act = act.astype(jnp.bfloat16)
        own_units = w_down.shape[0]
        return times(act[:, :own_units], w_down) + times(act[:, own_units:], other_down)

    def first_part():
        other_up, other_down, other_in = other_shards(0)
        rows_first = rows_at(picked, video_tokens[0])
        rows_cached = rows_at(picked, cached)
        scaled_first, _ = normalize(rows_first)
        own = from_everyone(scaled_first.astype(jnp.bfloat16), "fsdp_0")
        act_first, _ = gelu_both(up_both(own, other_up))
        columns_first = columns_of(own)
        routed = times(columns_first, paired_in(other_in))
        sums_first = jnp.concatenate([down_both(act_first, other_down), routed], axis=1)
        sums_first = summed_on_arrival(sums_first.astype(jnp.bfloat16), "fsdp_0")
        value_first, slope_first, gate_first = gate_of(sums_first[:, features:] + bias_row)
        change_first = rows_first + sums_first[:, :features] - rows_cached
        added_first = live * gate_first * change_first
        nothing = unset(
            (w_up.shape, w_up.dtype),
            (w_down.shape, w_down.dtype),
            ((features, hidden), r_in.dtype),
            ((group_rows, near_count * w_down.shape[0]), jnp.float32),
            ((group_rows, features), jnp.bfloat16),
        )
        passing = jnp.concatenate([added_first, change_first, picked], axis=1)
        state = (value_first, slope_first, gate_first, rows_cached, columns_first)
        return (passing, state, rows_cached, tuple(nothing))

    def second_waits():
        cot_rows = rows_at(picked, out_cotangent[0])
        piece = shard_cols // dp_count
        own_piece = lax.dynamic_slice_in_dim(r_in, lax.axis_index("dp") * piece, piece)
        sent = jnp.concatenate([cot_rows.astype(jnp.bfloat16), own_piece.reshape(1, features)])
        sent = from_everyone(sent, "fsdp_0")
        sent = sent.reshape(along_count, FRESH + 1, features)
        group = sent[:, :FRESH].reshape(group_rows, features)
        pieces = sent[:, FRESH].reshape(along_count * piece, hidden)
        other_up = halves_from_next(w_up)
        other_down = halves_from_next(w_down)
        whole_in = from_everyone(pieces, PLANE)
        whole_in = whole_in.reshape(near_count, dp_count, along_count, piece, hidden)
        whole_in = whole_in.transpose(2, 0, 1, 3, 4).reshape(features, hidden)
        act_grad = jnp.concatenate(
            [contract_last(group, w_down), contract_last(group, other_down)], axis=1
        )
        row = jnp.zeros((FRESH, hidden), jnp.float32)
        (columns,) = unset(((group_rows, pair_cols), jnp.bfloat16))
        state = (row, row, row[:, :1], rows_at(picked, cached), columns)
        passing = jnp.zeros((FRESH, 2 * features + picked.shape[1]), jnp.float32)
        return (passing, state, cot_rows, (other_up, other_down, whole_in, act_grad, group))

    passing, state, cot, others = lax.cond(second_section, second_waits, first_part)
    passed = lax.ppermute(passing, "pipe", [(0, 1)])
    cached_asked = rows_at(picked, cached_before)

    def second_part():
        other_up, other_down, whole_in, act_grad, cot_group = others
        rows_cached = state[3]
        match = contract_last(picked, passed[:, 2 * features :])

        def at_match(values):
            return match[:, :1] * values[:1] + match[:, 1:] * values[1:]

        rows_second = cached_asked + at_match(passed[:, :features])
        rows_second = rows_second.astype(jnp.bfloat16).astype(jnp.float32)
        moved = at_match(passed[:, features : 2 * features])
        scaled, inv_std = normalize(rows_second)
        tangent = inv_std * (
            moved
            - jnp.mean(moved, axis=1, keepdims=True)
            - scaled * jnp.mean(moved * scaled, axis=1, keepdims=True)
        )
        standing = jnp.sum(cot * (rows_second - rows_cached), axis=1, keepdims=True)
        moving = jnp.sum(cot * moved, axis=1, keepdims=True)
        numbers = jnp.concatenate(
            [live, match, *two_parts(standing), *two_parts(moving)], axis=1
        )
        numbers = jnp.pad(numbers, ((0, 0), (0, 128 - numbers.shape[1])))
        both = jnp.concatenate([scaled, tangent, numbers], axis=1).astype(jnp.bfloat16)
        both = from_everyone(both, "fsdp_0")
        stacked = jnp.concatenate([both[:, :features], both[:, features : 2 * features]])
        numbers = both[:, 2 * features :].astype(jnp.float32)
        pre_both = up_both(stacked, other_up)
        act, act_slope = gelu_both(pre_both[:group_rows])
        terms = down_both(act, other_down)
        block_parts = jnp.sum(terms * cot_group.astype(jnp.float32), axis=1)
        slope_parts = jnp.sum(act_grad * act_slope * pre_both[group_rows:], axis=1)
        parts = jnp.pad(jnp.stack([block_parts, slope_parts]), ((0, 0), (0, 128 - group_rows)))
        parts = jnp.broadcast_to(parts.astype(jnp.bfloat16), (along_count, *parts.shape))
        terms = terms.astype(jnp.bfloat16).reshape(along_count, FRESH, features)
        sums = summed_on_arrival(jnp.concatenate([terms, parts], axis=2), "fsdp_0")

        routed = times(stacked, whole_in)
        value, slope, gate = gate_of(routed[:group_rows] + bias_row)
        pull = r_out[None, :] * slope
        pull_tangent = jnp.sum(pull * routed[group_rows:], axis=1, keepdims=True)
        gate_own = lax.dynamic_slice_in_dim(gate, along * FRESH, FRESH)
        change = rows_second + sums[:, :features] - rows_cached
        live_group = numbers[:, :1]
        block_dot = sums[0, features : features + group_rows][:, None]
        slope_dot = sums[1, features : features + group_rows][:, None]
        gate_grad = live_group * (numbers[:, 3:4] + numbers[:, 4:5] + block_dot)
        logit_grad = gate_grad * gate * (1.0 - gate)
        input_grad = live_group * gate * (
            numbers[:, 5:6] + numbers[:, 6:7] + slope_dot
        ) + logit_grad * pull_tangent
        returning = (numbers[:, 1:3] * input_grad).reshape(along_count, FRESH, FRESH)
        return (
            jnp.sum(returning, axis=1).reshape(group_rows),
            rows_cached + live * gate_own * change,
            value,
            pull,
            logit_grad[:, 0],
            columns_of(stacked)[:group_rows],
        )

    def first_waits():
        value_first, slope_first, gate_first, rows_cached, columns_first = state
        factor = live * gate_first * (1.0 - gate_first)
        factors = jnp.pad(jnp.concatenate(two_parts(factor), axis=1), ((0, 0), (0, 126)))
        rows = jnp.concatenate([r_out[None, :] * slope_first, value_first, factors], axis=1)
        rows = from_everyone(rows.astype(jnp.bfloat16), "fsdp_0").astype(jnp.float32)
        return (
            jnp.zeros((group_rows,), jnp.float32),
            rows_cached + passing[:, :features],
            rows[:, hidden : 2 * hidden],
            rows[:, :hidden],
            rows[:, 2 * hidden] + rows[:, 2 * hidden + 1],
            columns_first,
        )

    returning, new_rows, value, pull, logit_grad, pair_columns = lax.cond(
        second_section, second_part, first_waits
    )

    returned = lax.ppermute(returning, "pipe", [(1, 0)])
    logit_grad = (jnp.where(second_section, 1.0, returned) * logit_grad)[:, None]
    hidden_rows = (logit_grad * pull).astype(jnp.bfloat16)
    out_row = jnp.sum(logit_grad * value, axis=0, keepdims=True)
    step_row = jnp.broadcast_to(timestep[0].astype(jnp.float32), (1, hidden))
    hidden_part = jnp.concatenate(
        [hidden_rows, out_row.astype(jnp.bfloat16), step_row.astype(jnp.bfloat16)]
    )
    shards = jnp.moveaxis(pair_columns.reshape(group_rows, near_count, shard_cols), 1, 0)
    shards = jnp.pad(shards, ((0, 0), (0, 2), (0, 128 - shard_cols)))
    message = jnp.concatenate(
        [jnp.broadcast_to(hidden_part, (near_count, *hidden_part.shape)), shards], axis=2
    )
    message = jnp.broadcast_to(message[:, None], (near_count, dp_count, *message.shape[1:]))
    arrived = lax.all_to_all(
        message.reshape(plane_count, *message.shape[2:]), PLANE, 0, 0, tiled=True
    )
    plane_rows = arrived[:, :group_rows].reshape(plane_count * group_rows, -1)
    hidden_rows = plane_rows[:, :hidden]
    summed_in = contract_first(plane_rows[:, hidden : hidden + shard_cols], hidden_rows)
    steps = jnp.arange(router_bias.shape[1]).astype(jnp.bfloat16)
    is_step = (steps[:, None] == arrived[:, group_rows + 1, 0][None, :]).astype(jnp.bfloat16)
    summed_bias = times(jnp.repeat(is_step, group_rows, axis=1), hidden_rows)
    summed_out = jnp.sum(arrived[:, group_rows, :hidden].astype(jnp.float32), axis=0)

    new_rows = new_rows.astype(jnp.bfloat16)
    blended = cached
    for row in range(FRESH):
        blended = jnp.where(picked[row][:, None] > 0, new_rows[row][None, :], blended)
    return (blended[None, None], summed_in[None], summed_bias[None], summed_out[None])


def solution(mesh):
    torus = Mesh(
        mesh.devices.reshape(16, 2, mesh.shape["pipe"], mesh.shape["dp"]),
        ("fsdp_0", "fsdp_1", "pipe", "dp"),
    )
    return jax.shard_map(
        body,
        mesh=torus,
        in_specs=(
            P("dp", FSDP, None),
            P("pipe", "dp", FSDP, None),
            P("pipe", "dp", FSDP),
            P("dp"),
            P("pipe", FSDP, None),
            P("pipe", FSDP, None),
            P("pipe", FSDP, None),
            P("pipe", None, None),
            P("pipe", None),
            P("dp", FSDP, None),
        ),
        out_specs=(
            P("pipe", "dp", FSDP, None),
            P("pipe", FSDP, None),
            P("pipe", None, None),
            P("pipe", None),
        ),
        check_vma=False,
    )
```

```python
import jax
import jax.numpy as jnp
from jax import lax
from jax.experimental import pallas as pl
from jax.sharding import Mesh
from jax.sharding import PartitionSpec as P


FRESH = 2
FSDP = ("fsdp_0", "fsdp_1")
PLANE = ("fsdp_1", "dp")


layer_eps = 1e-06
gelu_scale = 0.7978845608028654
gelu_cubic = 0.044715


def from_everyone(value, axis):
    copies = jnp.broadcast_to(value, (lax.axis_size(axis), *value.shape))
    arrived = lax.all_to_all(copies, axis, split_axis=0, concat_axis=0, tiled=True)
    return arrived.reshape(-1, value.shape[-1])


def summed_on_arrival(value, axis):
    blocks = value.reshape(lax.axis_size(axis), -1, value.shape[-1])
    arrived = lax.all_to_all(blocks, axis, split_axis=0, concat_axis=0, tiled=True)
    return arrived.astype(jnp.float32).sum(axis=0)


def gelu_both(values):
    inner_arg = gelu_scale * (values + gelu_cubic * values * values * values)
    tanh_val = jnp.tanh(inner_arg)
    half = 0.5 * (1.0 + tanh_val)
    slope = half + 0.5 * values * (1.0 - tanh_val * tanh_val) * gelu_scale * (
        1.0 + 3.0 * gelu_cubic * values * values
    )
    return (values * half, slope)


def normalize(inputs):
    values = inputs.astype(jnp.float32)
    center = values - jnp.mean(values, axis=1, keepdims=True)
    inv_std = lax.rsqrt(jnp.mean(center * center, axis=1, keepdims=True) + layer_eps)
    return (center * inv_std, inv_std)


def contract_last(left, right):
    return lax.dot_general(
        left, right, (((1,), (1,)), ((), ())), preferred_element_type=jnp.float32
    )


def contract_first(left, right):
    return lax.dot_general(
        left, right, (((0,), (0,)), ((), ())), preferred_element_type=jnp.float32
    )


def times(left, right):
    return jnp.dot(left, right, preferred_element_type=jnp.float32)


def two_parts(values):
    upper = lax.reduce_precision(values, exponent_bits=8, mantissa_bits=7)
    return [upper, values - upper]


def unset(*arrays):
    return pl.pallas_call(
        lambda *refs: None,
        out_shape=[jax.ShapeDtypeStruct(shape, dtype) for shape, dtype in arrays],
        out_specs=[pl.BlockSpec(memory_space=pl.ANY)] * len(arrays),
    )()


def pick_fresh(mask_row):
    rows = mask_row.shape[0]
    fresh = (mask_row > 0).astype(jnp.float32)
    before = (jnp.arange(rows)[:, None] <= jnp.arange(rows)[None, :]).astype(jnp.float32)
    rank = jnp.sum(before * fresh[:, None], axis=0)
    wanted = jnp.arange(1, FRESH + 1).astype(jnp.float32)
    return jnp.where(rank[None, :] == wanted[:, None], fresh[None, :], 0.0)


def rows_at(picked, values):
    return times(picked.astype(jnp.bfloat16), values)


def body(
    video_tokens,
    cached_out,
    fresh_mask,
    timestep,
    up_weight,
    down_weight,
    router_in,
    router_bias,
    router_out,
    out_cotangent,
):
    second_section = lax.axis_index("pipe") == 1
    near = lax.axis_index("fsdp_1")
    along = lax.axis_index("fsdp_0")
    column_slot = lax.axis_index(FSDP)
    cached = cached_out[0, 0]
    w_up = up_weight[0]
    w_down = down_weight[0]
    r_in = router_in[0]
    r_out = router_out[0]
    features = cached.shape[1]
    hidden = r_in.shape[1]
    shard_cols = r_in.shape[0]
    near_count = lax.axis_size("fsdp_1")
    along_count = lax.axis_size("fsdp_0")
    group_rows = along_count * FRESH
    dp_count = lax.axis_size("dp")
    plane_count = near_count * dp_count
    pair_cols = near_count * shard_cols
    bias_row = lax.dynamic_slice_in_dim(router_bias[0], timestep[0], 1)

    cached_before = lax.ppermute(cached, "pipe", [(0, 1)])
    picked = pick_fresh(fresh_mask[0, 0])
    live = jnp.sum(picked, axis=1, keepdims=True)

    def gate_of(router_pre):
        value, slope = gelu_both(router_pre)
        gate = jax.nn.sigmoid(jnp.sum(value * r_out[None, :], axis=1, keepdims=True))
        return (value, slope, gate)

    def columns_of(rows):
        return lax.dynamic_slice_in_dim(rows, along * pair_cols, pair_cols, 1)

    def from_next(value, section):
        place = lambda x_hi, dp: (x_hi * 2 + section) * dp_count + dp
        route = [
            (place(x_hi, dp), place(1 - x_hi, dp ^ (dp_count // 2)))
            for x_hi in range(near_count)
            for dp in range(dp_count)
        ]
        return lax.ppermute(value, ("fsdp_1", "pipe", "dp"), route)

    def up_both(rows, other_up):
        return jnp.concatenate([contract_last(rows, w_up), contract_last(rows, other_up)], axis=1)

    def down_both(act, other_down):
        act = act.astype(jnp.bfloat16)
        own_units = w_down.shape[0]
        return times(act[:, :own_units], w_down) + times(act[:, own_units:], other_down)

    def first_part():
        rows_first = rows_at(picked, video_tokens[0])
        rows_cached = rows_at(picked, cached)
        scaled_first, _ = normalize(rows_first)
        gathered = from_everyone(scaled_first.astype(jnp.bfloat16), FSDP)
        act_first, _ = gelu_both(contract_last(gathered, w_up))
        terms = times(act_first.astype(jnp.bfloat16), w_down)
        columns = lax.dynamic_slice_in_dim(gathered, column_slot * shard_cols, shard_cols, 1)
        sums_first = jnp.concatenate([terms, times(columns, r_in)], axis=1)
        sums_first = summed_on_arrival(sums_first.astype(jnp.bfloat16), FSDP)
        by_near = gathered.reshape(along_count, near_count, FRESH, features)
        group_first = lax.dynamic_index_in_dim(by_near, near, 1, keepdims=False)
        columns_first = columns_of(group_first.reshape(group_rows, features))
        value_first, slope_first, gate_first = gate_of(sums_first[:, features:] + bias_row)
        change_first = rows_first + sums_first[:, :features] - rows_cached
        added_first = live * gate_first * change_first
        nothing = unset(
            (w_up.shape, w_up.dtype),
            (w_down.shape, w_down.dtype),
            ((features, hidden), r_in.dtype),
            ((group_rows, near_count * w_down.shape[0]), jnp.float32),
            ((group_rows, features), jnp.bfloat16),
        )
        passing = jnp.concatenate([added_first, change_first, picked], axis=1)
        state = (value_first, slope_first, gate_first, rows_cached, columns_first)
        return (passing, state, rows_cached, tuple(nothing))

    def second_waits():
        cot_rows = rows_at(picked, out_cotangent[0])
        piece = shard_cols // dp_count
        own_piece = lax.dynamic_slice_in_dim(r_in, lax.axis_index("dp") * piece, piece)
        sent = jnp.concatenate([cot_rows.astype(jnp.bfloat16), own_piece.reshape(1, features)])
        sent = from_everyone(sent, "fsdp_0")
        sent = sent.reshape(along_count, FRESH + 1, features)
        group = sent[:, :FRESH].reshape(group_rows, features)
        pieces = sent[:, FRESH].reshape(along_count * piece, hidden)
        other_up = from_next(w_up, 1)
        other_down = from_next(w_down, 1)
        whole_in = from_everyone(pieces, PLANE)
        whole_in = whole_in.reshape(near_count, dp_count, along_count, piece, hidden)
        whole_in = whole_in.transpose(2, 0, 1, 3, 4).reshape(features, hidden)
        act_grad = jnp.concatenate(
            [contract_last(group, w_down), contract_last(group, other_down)], axis=1
        )
        row = jnp.zeros((FRESH, hidden), jnp.float32)
        (columns,) = unset(((group_rows, pair_cols), jnp.bfloat16))
        state = (row, row, row[:, :1], rows_at(picked, cached), columns)
        passing = jnp.zeros((FRESH, 2 * features + picked.shape[1]), jnp.float32)
        return (passing, state, cot_rows, (other_up, other_down, whole_in, act_grad, group))

    passing, state, cot, others = lax.cond(second_section, second_waits, first_part)
    passed = lax.ppermute(passing, "pipe", [(0, 1)])
    cached_asked = rows_at(picked, cached_before)

    def second_part():
        other_up, other_down, whole_in, act_grad, cot_group = others
        rows_cached = state[3]
        match = contract_last(picked, passed[:, 2 * features :])

        def at_match(values):
            return match[:, :1] * values[:1] + match[:, 1:] * values[1:]

        rows_second = cached_asked + at_match(passed[:, :features])
        rows_second = rows_second.astype(jnp.bfloat16).astype(jnp.float32)
        moved = at_match(passed[:, features : 2 * features])
        scaled, inv_std = normalize(rows_second)
        tangent = inv_std * (
            moved
            - jnp.mean(moved, axis=1, keepdims=True)
            - scaled * jnp.mean(moved * scaled, axis=1, keepdims=True)
        )
        standing = jnp.sum(cot * (rows_second - rows_cached), axis=1, keepdims=True)
        moving = jnp.sum(cot * moved, axis=1, keepdims=True)
        numbers = jnp.concatenate(
            [live, match, *two_parts(standing), *two_parts(moving)], axis=1
        )
        numbers = jnp.pad(numbers, ((0, 0), (0, 128 - numbers.shape[1])))
        both = jnp.concatenate([scaled, tangent, numbers], axis=1).astype(jnp.bfloat16)
        both = from_everyone(both, "fsdp_0")
        stacked = jnp.concatenate([both[:, :features], both[:, features : 2 * features]])
        numbers = both[:, 2 * features :].astype(jnp.float32)
        pre_both = up_both(stacked, other_up)
        act, act_slope = gelu_both(pre_both[:group_rows])
        terms = down_both(act, other_down)
        block_parts = jnp.sum(terms * cot_group.astype(jnp.float32), axis=1)
        slope_parts = jnp.sum(act_grad * act_slope * pre_both[group_rows:], axis=1)
        parts = jnp.pad(jnp.stack([block_parts, slope_parts]), ((0, 0), (0, 128 - group_rows)))
        parts = jnp.broadcast_to(parts.astype(jnp.bfloat16), (along_count, *parts.shape))
        terms = terms.astype(jnp.bfloat16).reshape(along_count, FRESH, features)
        sums = summed_on_arrival(jnp.concatenate([terms, parts], axis=2), "fsdp_0")

        routed = times(stacked, whole_in)
        value, slope, gate = gate_of(routed[:group_rows] + bias_row)
        pull = r_out[None, :] * slope
        pull_tangent = jnp.sum(pull * routed[group_rows:], axis=1, keepdims=True)
        gate_own = lax.dynamic_slice_in_dim(gate, along * FRESH, FRESH)
        change = rows_second + sums[:, :features] - rows_cached
        live_group = numbers[:, :1]
        block_dot = sums[0, features : features + group_rows][:, None]
        slope_dot = sums[1, features : features + group_rows][:, None]
        gate_grad = live_group * (numbers[:, 3:4] + numbers[:, 4:5] + block_dot)
        logit_grad = gate_grad * gate * (1.0 - gate)
        input_grad = live_group * gate * (
            numbers[:, 5:6] + numbers[:, 6:7] + slope_dot
        ) + logit_grad * pull_tangent
        returning = (numbers[:, 1:3] * input_grad).reshape(along_count, FRESH, FRESH)
        return (
            jnp.sum(returning, axis=1).reshape(group_rows),
            rows_cached + live * gate_own * change,
            value,
            pull,
            logit_grad[:, 0],
            columns_of(stacked)[:group_rows],
        )

    def first_waits():
        value_first, slope_first, gate_first, rows_cached, columns_first = state
        factor = live * gate_first * (1.0 - gate_first)
        factors = jnp.pad(jnp.concatenate(two_parts(factor), axis=1), ((0, 0), (0, 126)))
        rows = jnp.concatenate([r_out[None, :] * slope_first, value_first, factors], axis=1)
        rows = from_everyone(rows.astype(jnp.bfloat16), "fsdp_0").astype(jnp.float32)
        return (
            jnp.zeros((group_rows,), jnp.float32),
            rows_cached + passing[:, :features],
            rows[:, hidden : 2 * hidden],
            rows[:, :hidden],
            rows[:, 2 * hidden] + rows[:, 2 * hidden + 1],
            columns_first,
        )

    returning, new_rows, value, pull, logit_grad, pair_columns = lax.cond(
        second_section, second_part, first_waits
    )

    returned = lax.ppermute(returning, "pipe", [(1, 0)])
    logit_grad = (jnp.where(second_section, 1.0, returned) * logit_grad)[:, None]
    hidden_rows = (logit_grad * pull).astype(jnp.bfloat16)
    out_row = jnp.sum(logit_grad * value, axis=0, keepdims=True)
    step_row = jnp.broadcast_to(timestep[0].astype(jnp.float32), (1, hidden))
    hidden_part = jnp.concatenate(
        [hidden_rows, out_row.astype(jnp.bfloat16), step_row.astype(jnp.bfloat16)]
    )
    shards = jnp.moveaxis(pair_columns.reshape(group_rows, near_count, shard_cols), 1, 0)
    shards = jnp.pad(shards, ((0, 0), (0, 2), (0, 128 - shard_cols)))
    message = jnp.concatenate(
        [jnp.broadcast_to(hidden_part, (near_count, *hidden_part.shape)), shards], axis=2
    )
    message = jnp.broadcast_to(message[:, None], (near_count, dp_count, *message.shape[1:]))
    arrived = lax.all_to_all(
        message.reshape(plane_count, *message.shape[2:]), PLANE, 0, 0, tiled=True
    )
    plane_rows = arrived[:, :group_rows].reshape(plane_count * group_rows, -1)
    hidden_rows = plane_rows[:, :hidden]
    summed_in = contract_first(plane_rows[:, hidden : hidden + shard_cols], hidden_rows)
    steps = jnp.arange(router_bias.shape[1]).astype(jnp.bfloat16)
    is_step = (steps[:, None] == arrived[:, group_rows + 1, 0][None, :]).astype(jnp.bfloat16)
    summed_bias = times(jnp.repeat(is_step, group_rows, axis=1), hidden_rows)
    summed_out = jnp.sum(arrived[:, group_rows, :hidden].astype(jnp.float32), axis=0)

    new_rows = new_rows.astype(jnp.bfloat16)
    blended = cached
    for row in range(FRESH):
        blended = jnp.where(picked[row][:, None] > 0, new_rows[row][None, :], blended)
    return (blended[None, None], summed_in[None], summed_bias[None], summed_out[None])


def solution(mesh):
    torus = Mesh(
        mesh.devices.reshape(16, 2, mesh.shape["pipe"], mesh.shape["dp"]),
        ("fsdp_0", "fsdp_1", "pipe", "dp"),
    )
    return jax.shard_map(
        body,
        mesh=torus,
        in_specs=(
            P("dp", FSDP, None),
            P("pipe", "dp", FSDP, None),
            P("pipe", "dp", FSDP),
            P("dp"),
            P("pipe", FSDP, None),
            P("pipe", FSDP, None),
            P("pipe", FSDP, None),
            P("pipe", None, None),
            P("pipe", None),
            P("dp", FSDP, None),
        ),
        out_specs=(
            P("pipe", "dp", FSDP, None),
            P("pipe", FSDP, None),
            P("pipe", None, None),
            P("pipe", None),
        ),
        check_vma=False,
    )
```

```python
import jax
import jax.numpy as jnp
from jax import lax
from jax.experimental import pallas as pl
from jax.experimental.pallas import tpu as pltpu
from jax.sharding import Mesh
from jax.sharding import PartitionSpec as P


FRESH = 2
FSDP = ("fsdp_0", "fsdp_1")
PLANE = ("fsdp_1", "dp")


layer_eps = 1e-06
gelu_scale = 0.7978845608028654
gelu_cubic = 0.044715


def from_everyone(value, axis):
    copies = jnp.broadcast_to(value, (lax.axis_size(axis), *value.shape))
    arrived = lax.all_to_all(copies, axis, split_axis=0, concat_axis=0, tiled=True)
    return arrived.reshape(-1, value.shape[-1])


def summed_on_arrival(value, axis):
    blocks = value.reshape(lax.axis_size(axis), -1, value.shape[-1])
    arrived = lax.all_to_all(blocks, axis, split_axis=0, concat_axis=0, tiled=True)
    return arrived.astype(jnp.float32).sum(axis=0)


def gelu_both(values):
    inner_arg = gelu_scale * (values + gelu_cubic * values * values * values)
    tanh_val = jnp.tanh(inner_arg)
    half = 0.5 * (1.0 + tanh_val)
    slope = half + 0.5 * values * (1.0 - tanh_val * tanh_val) * gelu_scale * (
        1.0 + 3.0 * gelu_cubic * values * values
    )
    return (values * half, slope)


def normalize(inputs):
    values = inputs.astype(jnp.float32)
    center = values - jnp.mean(values, axis=1, keepdims=True)
    inv_std = lax.rsqrt(jnp.mean(center * center, axis=1, keepdims=True) + layer_eps)
    return (center * inv_std, inv_std)


def contract_last(left, right):
    return lax.dot_general(
        left, right, (((1,), (1,)), ((), ())), preferred_element_type=jnp.float32
    )


def contract_first(left, right):
    return lax.dot_general(
        left, right, (((0,), (0,)), ((), ())), preferred_element_type=jnp.float32
    )


def times(left, right):
    return jnp.dot(left, right, preferred_element_type=jnp.float32)


def two_parts(values):
    upper = lax.reduce_precision(values, exponent_bits=8, mantissa_bits=7)
    return [upper, values - upper]


def unset(*arrays):
    return pl.pallas_call(
        lambda *refs: None,
        out_shape=[jax.ShapeDtypeStruct(shape, dtype) for shape, dtype in arrays],
        out_specs=[pl.BlockSpec(memory_space=pl.ANY)] * len(arrays),
    )()


def final_message(flags, returned, logit, pull, value, shards, plane_count):
    rows, hidden = pull.shape
    per_shard = plane_count // shards.shape[0]
    lanes = shards.shape[2]

    def kernel(flags_ref, returned_ref, logit_ref, pull_ref, value_ref, shards_ref, out_ref):
        scale = jnp.where(flags_ref[0] > 0, 1.0, returned_ref[...])
        grads = logit_ref[...] * scale
        hidden_rows = (grads * pull_ref[...]).astype(jnp.bfloat16)
        out_row = jnp.sum(grads * value_ref[...], axis=0, keepdims=True)
        place = lax.broadcasted_iota(jnp.int32, (8, hidden), 0)
        tail = jnp.where(place == 0, out_row, jnp.where(place == 1, flags_ref[1], 0.0))
        tail = tail.astype(jnp.bfloat16)
        for target in range(plane_count):
            out_ref[target, :rows, :hidden] = hidden_rows
            out_ref[target, :rows, hidden:] = shards_ref[target // per_shard]
            out_ref[target, rows:, :hidden] = tail
            out_ref[target, rows:, hidden:] = jnp.zeros((8, lanes), jnp.bfloat16)

    vmem = pl.BlockSpec(memory_space=pltpu.VMEM)
    return pl.pallas_call(
        kernel,
        out_shape=jax.ShapeDtypeStruct((plane_count, rows + 8, hidden + lanes), jnp.bfloat16),
        in_specs=[pl.BlockSpec(memory_space=pltpu.SMEM)] + [vmem] * 5,
        out_specs=vmem,
    )(flags, returned, logit, pull, value, shards)


def final_sums(arrived, rows, hidden, shard_cols, step_count):
    plane_count = arrived.shape[0]

    def kernel(arrived_ref, in_ref, bias_ref, out_ref):
        place = lax.broadcasted_iota(jnp.int32, (step_count, hidden), 0).astype(jnp.float32)
        in_sum = jnp.zeros((arrived.shape[2] - hidden, hidden), jnp.float32)
        bias_sum = jnp.zeros((step_count, hidden), jnp.float32)
        out_sum = jnp.zeros((1, hidden), jnp.float32)
        for source in range(plane_count):
            hidden_rows = arrived_ref[source, :rows, :hidden]
            in_sum += contract_first(arrived_ref[source, :rows, hidden:], hidden_rows)
            tail = arrived_ref[source, rows:, :hidden].astype(jnp.float32)
            total = jnp.sum(hidden_rows.astype(jnp.float32), axis=0, keepdims=True)
            bias_sum += jnp.where(place == tail[1:2], total, 0.0)
            out_sum += tail[:1]
        in_ref[...] = in_sum[:shard_cols]
        bias_ref[...] = bias_sum
        out_ref[...] = out_sum

    vmem = pl.BlockSpec(memory_space=pltpu.VMEM)
    shapes = [(shard_cols, hidden), (step_count, hidden), (1, hidden)]
    return pl.pallas_call(
        kernel,
        out_shape=[jax.ShapeDtypeStruct(shape, jnp.float32) for shape in shapes],
        in_specs=[vmem],
        out_specs=[vmem] * 3,
    )(arrived)


def pick_fresh(mask_row):
    rows = mask_row.shape[0]
    fresh = (mask_row > 0).astype(jnp.float32)
    before = (jnp.arange(rows)[:, None] <= jnp.arange(rows)[None, :]).astype(jnp.float32)
    rank = jnp.sum(before * fresh[:, None], axis=0)
    wanted = jnp.arange(1, FRESH + 1).astype(jnp.float32)
    return jnp.where(rank[None, :] == wanted[:, None], fresh[None, :], 0.0)


def rows_at(picked, values):
    return times(picked.astype(jnp.bfloat16), values)


def body(
    video_tokens,
    cached_out,
    fresh_mask,
    timestep,
    up_weight,
    down_weight,
    router_in,
    router_bias,
    router_out,
    out_cotangent,
):
    second_section = lax.axis_index("pipe") == 1
    near = lax.axis_index("fsdp_1")
    along = lax.axis_index("fsdp_0")
    column_slot = lax.axis_index(FSDP)
    cached = cached_out[0, 0]
    w_up = up_weight[0]
    w_down = down_weight[0]
    r_in = router_in[0]
    r_out = router_out[0]
    features = cached.shape[1]
    hidden = r_in.shape[1]
    shard_cols = r_in.shape[0]
    near_count = lax.axis_size("fsdp_1")
    along_count = lax.axis_size("fsdp_0")
    group_rows = along_count * FRESH
    dp_count = lax.axis_size("dp")
    plane_count = near_count * dp_count
    pair_cols = near_count * shard_cols
    bias_row = lax.dynamic_slice_in_dim(router_bias[0], timestep[0], 1)

    cached_before = lax.ppermute(cached, "pipe", [(0, 1)])
    picked = pick_fresh(fresh_mask[0, 0])
    live = jnp.sum(picked, axis=1, keepdims=True)

    def gate_of(router_pre):
        value, slope = gelu_both(router_pre)
        gate = jax.nn.sigmoid(jnp.sum(value * r_out[None, :], axis=1, keepdims=True))
        return (value, slope, gate)

    def columns_of(rows):
        return lax.dynamic_slice_in_dim(rows, along * pair_cols, pair_cols, 1)

    def from_next(value, section):
        place = lambda x_hi, dp: (x_hi * 2 + section) * dp_count + dp
        route = [
            (place(x_hi, dp), place(1 - x_hi, dp ^ (dp_count // 2)))
            for x_hi in range(near_count)
            for dp in range(dp_count)
        ]
        return lax.ppermute(value, ("fsdp_1", "pipe", "dp"), route)

    def up_both(rows, other_up):
        return jnp.concatenate([contract_last(rows, w_up), contract_last(rows, other_up)], axis=1)

    def down_both(act, other_down):
        act = act.astype(jnp.bfloat16)
        own_units = w_down.shape[0]
        return times(act[:, :own_units], w_down) + times(act[:, own_units:], other_down)

    def shards_of(columns):
        shards = jnp.moveaxis(columns.reshape(group_rows, near_count, shard_cols), 1, 0)
        return jnp.pad(shards, ((0, 0), (0, 0), (0, 128 - shard_cols)))

    def first_part():
        rows_first = rows_at(picked, video_tokens[0])
        rows_cached = rows_at(picked, cached)
        scaled_first, _ = normalize(rows_first)
        gathered = from_everyone(scaled_first.astype(jnp.bfloat16), FSDP)
        act_first, _ = gelu_both(contract_last(gathered, w_up))
        terms = times(act_first.astype(jnp.bfloat16), w_down)
        columns = lax.dynamic_slice_in_dim(gathered, column_slot * shard_cols, shard_cols, 1)
        sums_first = jnp.concatenate([terms, times(columns, r_in)], axis=1)
        sums_first = summed_on_arrival(sums_first.astype(jnp.bfloat16), FSDP)
        by_near = gathered.reshape(along_count, near_count, FRESH, features)
        group_first = lax.dynamic_index_in_dim(by_near, near, 1, keepdims=False)
        columns_first = columns_of(group_first.reshape(group_rows, features))
        value_first, slope_first, gate_first = gate_of(sums_first[:, features:] + bias_row)
        change_first = rows_first + sums_first[:, :features] - rows_cached
        added_first = live * gate_first * change_first
        nothing = unset(
            (w_up.shape, w_up.dtype),
            (w_down.shape, w_down.dtype),
            ((features, hidden), r_in.dtype),
            ((group_rows, near_count * w_down.shape[0]), jnp.float32),
            ((group_rows, features), jnp.bfloat16),
        )
        passing = jnp.concatenate([added_first, change_first, picked], axis=1)
        state = (value_first, slope_first, gate_first, rows_cached, columns_first)
        return (passing, state, rows_cached, tuple(nothing))

    def second_waits():
        cot_rows = rows_at(picked, out_cotangent[0])
        piece = shard_cols // dp_count
        own_piece = lax.dynamic_slice_in_dim(r_in, lax.axis_index("dp") * piece, piece)
        sent = jnp.concatenate([cot_rows.astype(jnp.bfloat16), own_piece.reshape(1, features)])
        sent = from_everyone(sent, "fsdp_0")
        sent = sent.reshape(along_count, FRESH + 1, features)
        group = sent[:, :FRESH].reshape(group_rows, features)
        pieces = sent[:, FRESH].reshape(along_count * piece, hidden)
        other_up = from_next(w_up, 1)
        other_down = from_next(w_down, 1)
        whole_in = from_everyone(pieces, PLANE)
        act_grad = jnp.concatenate(
            [contract_last(group, w_down), contract_last(group, other_down)], axis=1
        )
        row = jnp.zeros((FRESH, hidden), jnp.float32)
        (columns,) = unset(((group_rows, pair_cols), jnp.bfloat16))
        state = (row, row, row[:, :1], rows_at(picked, cached), columns)
        passing = jnp.zeros((FRESH, 2 * features + picked.shape[1]), jnp.float32)
        return (passing, state, cot_rows, (other_up, other_down, whole_in, act_grad, group))

    passing, state, cot, others = lax.cond(second_section, second_waits, first_part)
    passed = lax.ppermute(passing, "pipe", [(0, 1)])
    cached_asked = rows_at(picked, cached_before)

    def second_part():
        other_up, other_down, whole_in, act_grad, cot_group = others
        rows_cached = state[3]
        match = contract_last(picked, passed[:, 2 * features :])

        def at_match(values):
            return match[:, :1] * values[:1] + match[:, 1:] * values[1:]

        rows_second = cached_asked + at_match(passed[:, :features])
        rows_second = rows_second.astype(jnp.bfloat16).astype(jnp.float32)
        moved = at_match(passed[:, features : 2 * features])
        scaled, inv_std = normalize(rows_second)
        tangent = inv_std * (
            moved
            - jnp.mean(moved, axis=1, keepdims=True)
            - scaled * jnp.mean(moved * scaled, axis=1, keepdims=True)
        )
        standing = jnp.sum(cot * (rows_second - rows_cached), axis=1, keepdims=True)
        moving = jnp.sum(cot * moved, axis=1, keepdims=True)
        numbers = jnp.concatenate(
            [live, match, *two_parts(standing), *two_parts(moving)], axis=1
        )
        numbers = jnp.pad(numbers, ((0, 0), (0, 128 - numbers.shape[1])))
        both = jnp.concatenate([scaled, tangent, numbers], axis=1).astype(jnp.bfloat16)
        both = from_everyone(both, "fsdp_0")
        stacked = jnp.concatenate([both[:, :features], both[:, features : 2 * features]])
        numbers = both[:, 2 * features :].astype(jnp.float32)
        pre_both = up_both(stacked, other_up)
        act, act_slope = gelu_both(pre_both[:group_rows])
        terms = down_both(act, other_down)
        block_parts = jnp.sum(terms * cot_group.astype(jnp.float32), axis=1)
        slope_parts = jnp.sum(act_grad * act_slope * pre_both[group_rows:], axis=1)
        parts = jnp.pad(jnp.stack([block_parts, slope_parts]), ((0, 0), (0, 128 - group_rows)))
        parts = jnp.broadcast_to(parts.astype(jnp.bfloat16), (along_count, *parts.shape))
        terms = terms.astype(jnp.bfloat16).reshape(along_count, FRESH, features)
        sums = summed_on_arrival(jnp.concatenate([terms, parts], axis=2), "fsdp_0")

        piece = shard_cols // dp_count
        whole_in = whole_in.reshape(near_count, dp_count, along_count, piece, hidden)
        whole_in = whole_in.transpose(2, 0, 1, 3, 4).reshape(features, hidden)
        routed = times(stacked, whole_in)
        value, slope, gate = gate_of(routed[:group_rows] + bias_row)
        pull = r_out[None, :] * slope
        pull_tangent = jnp.sum(pull * routed[group_rows:], axis=1, keepdims=True)
        gate_own = lax.dynamic_slice_in_dim(gate, along * FRESH, FRESH)
        change = rows_second + sums[:, :features] - rows_cached
        live_group = numbers[:, :1]
        block_dot = sums[0, features : features + group_rows][:, None]
        slope_dot = sums[1, features : features + group_rows][:, None]
        gate_grad = live_group * (numbers[:, 3:4] + numbers[:, 4:5] + block_dot)
        logit_grad = gate_grad * gate * (1.0 - gate)
        input_grad = live_group * gate * (
            numbers[:, 5:6] + numbers[:, 6:7] + slope_dot
        ) + logit_grad * pull_tangent
        by_first = numbers[:, 1:3] * input_grad
        even = (jnp.arange(group_rows) % FRESH == 0)[:, None]
        partner = jnp.where(even, jnp.roll(by_first, -1, axis=0), jnp.roll(by_first, 1, axis=0))
        by_first = by_first + partner
        return (
            jnp.where(even, by_first[:, :1], by_first[:, 1:]),
            rows_cached + live * gate_own * change,
            value,
            pull,
            logit_grad,
            shards_of(columns_of(stacked[:group_rows])),
        )

    def first_waits():
        value_first, slope_first, gate_first, rows_cached, columns_first = state
        factor = live * gate_first * (1.0 - gate_first)
        factors = jnp.pad(jnp.concatenate(two_parts(factor), axis=1), ((0, 0), (0, 126)))
        rows = jnp.concatenate([r_out[None, :] * slope_first, value_first, factors], axis=1)
        rows = from_everyone(rows.astype(jnp.bfloat16), "fsdp_0").astype(jnp.float32)
        return (
            jnp.zeros((group_rows, 1), jnp.float32),
            rows_cached + passing[:, :features],
            rows[:, hidden : 2 * hidden],
            rows[:, :hidden],
            rows[:, 2 * hidden : 2 * hidden + 1] + rows[:, 2 * hidden + 1 : 2 * hidden + 2],
            shards_of(columns_first),
        )

    returning, new_rows, value, pull, logit_grad, shards = lax.cond(
        second_section, second_part, first_waits
    )

    returned = lax.ppermute(returning, "pipe", [(1, 0)])
    flags = jnp.stack([second_section.astype(jnp.float32), timestep[0].astype(jnp.float32)])
    message = final_message(flags, returned, logit_grad, pull, value, shards, plane_count)
    arrived = lax.all_to_all(message, PLANE, split_axis=0, concat_axis=0, tiled=True)
    summed_in, summed_bias, summed_out = final_sums(
        arrived, group_rows, hidden, shard_cols, router_bias.shape[1]
    )

    new_rows = new_rows.astype(jnp.bfloat16)
    blended = cached
    for row in range(FRESH):
        blended = jnp.where(picked[row][:, None] > 0, new_rows[row][None, :], blended)
    return (blended[None, None], summed_in[None], summed_bias[None], summed_out)


def solution(mesh):
    torus = Mesh(
        mesh.devices.reshape(16, 2, mesh.shape["pipe"], mesh.shape["dp"]),
        ("fsdp_0", "fsdp_1", "pipe", "dp"),
    )
    return jax.shard_map(
        body,
        mesh=torus,
        in_specs=(
            P("dp", FSDP, None),
            P("pipe", "dp", FSDP, None),
            P("pipe", "dp", FSDP),
            P("dp"),
            P("pipe", FSDP, None),
            P("pipe", FSDP, None),
            P("pipe", FSDP, None),
            P("pipe", None, None),
            P("pipe", None),
            P("dp", FSDP, None),
        ),
        out_specs=(
            P("pipe", "dp", FSDP, None),
            P("pipe", FSDP, None),
            P("pipe", None, None),
            P("pipe", None),
        ),
        check_vma=False,
    )
```

```python
import jax
import jax.numpy as jnp
from jax import lax
from jax.experimental import pallas as pl
from jax.experimental.pallas import tpu as pltpu
from jax.sharding import Mesh
from jax.sharding import PartitionSpec as P


FRESH = 2
FSDP = ("fsdp_0", "fsdp_1")
PLANE = ("fsdp_1", "dp")


layer_eps = 1e-06
gelu_scale = 0.7978845608028654
gelu_cubic = 0.044715


def from_everyone(value, axis):
    copies = jnp.broadcast_to(value, (lax.axis_size(axis), *value.shape))
    arrived = lax.all_to_all(copies, axis, split_axis=0, concat_axis=0, tiled=True)
    return arrived.reshape(-1, value.shape[-1])


def summed_on_arrival(value, axis):
    blocks = value.reshape(lax.axis_size(axis), -1, value.shape[-1])
    arrived = lax.all_to_all(blocks, axis, split_axis=0, concat_axis=0, tiled=True)
    return arrived.astype(jnp.float32).sum(axis=0)


def gelu_both(values):
    inner_arg = gelu_scale * (values + gelu_cubic * values * values * values)
    tanh_val = jnp.tanh(inner_arg)
    half = 0.5 * (1.0 + tanh_val)
    slope = half + 0.5 * values * (1.0 - tanh_val * tanh_val) * gelu_scale * (
        1.0 + 3.0 * gelu_cubic * values * values
    )
    return (values * half, slope)


def normalize(inputs):
    values = inputs.astype(jnp.float32)
    center = values - jnp.mean(values, axis=1, keepdims=True)
    inv_std = lax.rsqrt(jnp.mean(center * center, axis=1, keepdims=True) + layer_eps)
    return (center * inv_std, inv_std)


def contract_last(left, right):
    return lax.dot_general(
        left, right, (((1,), (1,)), ((), ())), preferred_element_type=jnp.float32
    )


def contract_first(left, right):
    return lax.dot_general(
        left, right, (((0,), (0,)), ((), ())), preferred_element_type=jnp.float32
    )


def times(left, right):
    return jnp.dot(left, right, preferred_element_type=jnp.float32)


def two_parts(values):
    upper = lax.reduce_precision(values, exponent_bits=8, mantissa_bits=7)
    return [upper, values - upper]


def unset(*arrays):
    return pl.pallas_call(
        lambda *refs: None,
        out_shape=[jax.ShapeDtypeStruct(shape, dtype) for shape, dtype in arrays],
        out_specs=[pl.BlockSpec(memory_space=pl.ANY)] * len(arrays),
    )()


def final_message(flags, returned, logit, pull, value, shards, plane_count):
    rows, hidden = pull.shape
    per_shard = plane_count // shards.shape[0]
    lanes = shards.shape[2]

    def kernel(flags_ref, returned_ref, logit_ref, pull_ref, value_ref, shards_ref, out_ref):
        scale = jnp.where(flags_ref[0] > 0, 1.0, returned_ref[...])
        square = [lax.broadcasted_iota(jnp.int32, (rows, rows), axis) for axis in (0, 1)]
        spread = jnp.where(square[0] == square[1], logit_ref[...] * scale, 0.0)
        grads = jnp.sum(spread, axis=1, keepdims=True)
        hidden_rows = (grads * pull_ref[...]).astype(jnp.bfloat16)
        out_row = jnp.sum(grads * value_ref[...], axis=0, keepdims=True)
        place = lax.broadcasted_iota(jnp.int32, (8, hidden), 0)
        tail = jnp.where(place == 0, out_row, jnp.where(place == 1, flags_ref[1], 0.0))
        tail = tail.astype(jnp.bfloat16)
        for target in range(plane_count):
            out_ref[target, :rows, :hidden] = hidden_rows
            out_ref[target, :rows, hidden:] = shards_ref[target // per_shard]
            out_ref[target, rows:, :hidden] = tail
            out_ref[target, rows:, hidden:] = jnp.zeros((8, lanes), jnp.bfloat16)

    vmem = pl.BlockSpec(memory_space=pltpu.VMEM)
    return pl.pallas_call(
        kernel,
        out_shape=jax.ShapeDtypeStruct((plane_count, rows + 8, hidden + lanes), jnp.bfloat16),
        in_specs=[pl.BlockSpec(memory_space=pltpu.SMEM)] + [vmem] * 5,
        out_specs=vmem,
    )(flags, returned[None], logit[None], pull, value, shards)


def pick_fresh(mask_row):
    rows = mask_row.shape[0]
    fresh = (mask_row > 0).astype(jnp.float32)
    before = (jnp.arange(rows)[:, None] <= jnp.arange(rows)[None, :]).astype(jnp.float32)
    rank = jnp.sum(before * fresh[:, None], axis=0)
    wanted = jnp.arange(1, FRESH + 1).astype(jnp.float32)
    return jnp.where(rank[None, :] == wanted[:, None], fresh[None, :], 0.0)


def rows_at(picked, values):
    return times(picked.astype(jnp.bfloat16), values)


def body(
    video_tokens,
    cached_out,
    fresh_mask,
    timestep,
    up_weight,
    down_weight,
    router_in,
    router_bias,
    router_out,
    out_cotangent,
):
    second_section = lax.axis_index("pipe") == 1
    near = lax.axis_index("fsdp_1")
    along = lax.axis_index("fsdp_0")
    column_slot = lax.axis_index(FSDP)
    cached = cached_out[0, 0]
    w_up = up_weight[0]
    w_down = down_weight[0]
    r_in = router_in[0]
    r_out = router_out[0]
    features = cached.shape[1]
    hidden = r_in.shape[1]
    shard_cols = r_in.shape[0]
    near_count = lax.axis_size("fsdp_1")
    along_count = lax.axis_size("fsdp_0")
    group_rows = along_count * FRESH
    dp_count = lax.axis_size("dp")
    plane_count = near_count * dp_count
    pair_cols = near_count * shard_cols
    bias_row = lax.dynamic_slice_in_dim(router_bias[0], timestep[0], 1)

    cached_before = lax.ppermute(cached, "pipe", [(0, 1)])
    picked = pick_fresh(fresh_mask[0, 0])
    live = jnp.sum(picked, axis=1, keepdims=True)

    def gate_of(router_pre):
        value, slope = gelu_both(router_pre)
        gate = jax.nn.sigmoid(jnp.sum(value * r_out[None, :], axis=1, keepdims=True))
        return (value, slope, gate)

    def columns_of(rows):
        return lax.dynamic_slice_in_dim(rows, along * pair_cols, pair_cols, 1)

    def from_next(value, section):
        place = lambda x_hi, dp: (x_hi * 2 + section) * dp_count + dp
        route = [
            (place(x_hi, dp), place(1 - x_hi, dp ^ (dp_count // 2)))
            for x_hi in range(near_count)
            for dp in range(dp_count)
        ]
        return lax.ppermute(value, ("fsdp_1", "pipe", "dp"), route)

    def up_both(rows, other_up):
        return jnp.concatenate([contract_last(rows, w_up), contract_last(rows, other_up)], axis=1)

    def down_both(act, other_down):
        act = act.astype(jnp.bfloat16)
        own_units = w_down.shape[0]
        return times(act[:, :own_units], w_down) + times(act[:, own_units:], other_down)

    def shards_of(columns):
        shards = jnp.moveaxis(columns.reshape(group_rows, near_count, shard_cols), 1, 0)
        return jnp.pad(shards, ((0, 0), (0, 0), (0, 128 - shard_cols)))

    def first_part():
        rows_first = rows_at(picked, video_tokens[0])
        rows_cached = rows_at(picked, cached)
        scaled_first, _ = normalize(rows_first)
        gathered = from_everyone(scaled_first.astype(jnp.bfloat16), FSDP)
        act_first, _ = gelu_both(contract_last(gathered, w_up))
        terms = times(act_first.astype(jnp.bfloat16), w_down)
        columns = lax.dynamic_slice_in_dim(gathered, column_slot * shard_cols, shard_cols, 1)
        sums_first = jnp.concatenate([terms, times(columns, r_in)], axis=1)
        sums_first = summed_on_arrival(sums_first.astype(jnp.bfloat16), FSDP)
        by_near = gathered.reshape(along_count, near_count, FRESH, features)
        group_first = lax.dynamic_index_in_dim(by_near, near, 1, keepdims=False)
        columns_first = columns_of(group_first.reshape(group_rows, features))
        value_first, slope_first, gate_first = gate_of(sums_first[:, features:] + bias_row)
        change_first = rows_first + sums_first[:, :features] - rows_cached
        added_first = live * gate_first * change_first
        nothing = unset(
            (w_up.shape, w_up.dtype),
            (w_down.shape, w_down.dtype),
            ((features, hidden), r_in.dtype),
            ((group_rows, near_count * w_down.shape[0]), jnp.float32),
            ((group_rows, features), jnp.bfloat16),
        )
        passing = jnp.concatenate([added_first, change_first, picked], axis=1)
        state = (value_first, slope_first, gate_first, rows_cached, columns_first)
        return (passing, state, rows_cached, tuple(nothing))

    def second_waits():
        cot_rows = rows_at(picked, out_cotangent[0])
        piece = shard_cols // dp_count
        own_piece = lax.dynamic_slice_in_dim(r_in, lax.axis_index("dp") * piece, piece)
        sent = jnp.concatenate([cot_rows.astype(jnp.bfloat16), own_piece.reshape(1, features)])
        sent = from_everyone(sent, "fsdp_0")
        sent = sent.reshape(along_count, FRESH + 1, features)
        group = sent[:, :FRESH].reshape(group_rows, features)
        pieces = sent[:, FRESH].reshape(along_count * piece, hidden)
        half = w_up.shape[0] // 2
        other_up = from_next(w_up[:half], 1)
        other_up = jnp.concatenate([other_up, from_next(w_up[half:], 1)])
        other_down = from_next(w_down, 1)
        whole_in = from_everyone(pieces, PLANE)
        act_grad = jnp.concatenate(
            [contract_last(group, w_down), contract_last(group, other_down)], axis=1
        )
        row = jnp.zeros((FRESH, hidden), jnp.float32)
        (columns,) = unset(((group_rows, pair_cols), jnp.bfloat16))
        state = (row, row, row[:, :1], rows_at(picked, cached), columns)
        passing = jnp.zeros((FRESH, 2 * features + picked.shape[1]), jnp.float32)
        return (passing, state, cot_rows, (other_up, other_down, whole_in, act_grad, group))

    passing, state, cot, others = lax.cond(second_section, second_waits, first_part)
    passed = lax.ppermute(passing, "pipe", [(0, 1)])
    cached_asked = rows_at(picked, cached_before)

    def second_part():
        other_up, other_down, whole_in, act_grad, cot_group = others
        rows_cached = state[3]
        match = contract_last(picked, passed[:, 2 * features :])

        def at_match(values):
            return match[:, :1] * values[:1] + match[:, 1:] * values[1:]

        rows_second = cached_asked + at_match(passed[:, :features])
        rows_second = rows_second.astype(jnp.bfloat16).astype(jnp.float32)
        moved = at_match(passed[:, features : 2 * features])
        scaled, inv_std = normalize(rows_second)
        tangent = inv_std * (
            moved
            - jnp.mean(moved, axis=1, keepdims=True)
            - scaled * jnp.mean(moved * scaled, axis=1, keepdims=True)
        )
        standing = jnp.sum(cot * (rows_second - rows_cached), axis=1, keepdims=True)
        moving = jnp.sum(cot * moved, axis=1, keepdims=True)
        numbers = jnp.concatenate(
            [live, match, *two_parts(standing), *two_parts(moving)], axis=1
        )
        numbers = jnp.pad(numbers, ((0, 0), (0, 128 - numbers.shape[1])))
        both = jnp.concatenate([scaled, tangent, numbers], axis=1).astype(jnp.bfloat16)
        both = from_everyone(both, "fsdp_0")
        stacked = jnp.concatenate([both[:, :features], both[:, features : 2 * features]])
        numbers = both[:, 2 * features : 2 * features + 8].astype(jnp.float32).T
        pre_both = up_both(stacked, other_up)
        act, act_slope = gelu_both(pre_both[:group_rows])
        terms = down_both(act, other_down)
        block_parts = jnp.sum(terms * cot_group.astype(jnp.float32), axis=1)
        slope_parts = jnp.sum(act_grad * act_slope * pre_both[group_rows:], axis=1)
        parts = jnp.pad(jnp.stack([block_parts, slope_parts]), ((0, 0), (0, 128 - group_rows)))
        parts = jnp.broadcast_to(parts.astype(jnp.bfloat16), (along_count, *parts.shape))
        terms = terms.astype(jnp.bfloat16).reshape(along_count, FRESH, features)
        sums = summed_on_arrival(jnp.concatenate([terms, parts], axis=2), "fsdp_0")

        piece = shard_cols // dp_count
        whole_in = whole_in.reshape(near_count, dp_count, along_count, piece, hidden)
        whole_in = whole_in.transpose(2, 0, 1, 3, 4).reshape(features, hidden)
        routed = times(stacked, whole_in)
        value, slope, gate = gate_of(routed[:group_rows] + bias_row)
        pull = r_out[None, :] * slope
        pull_tangent = jnp.sum(pull * routed[group_rows:], axis=1)
        gate_own = lax.dynamic_slice_in_dim(gate, along * FRESH, FRESH)
        change = rows_second + sums[:, :features] - rows_cached
        gate = gate[:, 0]
        block_dot = sums[0, features : features + group_rows]
        slope_dot = sums[1, features : features + group_rows]
        gate_grad = numbers[0] * (numbers[3] + numbers[4] + block_dot)
        logit_grad = gate_grad * gate * (1.0 - gate)
        input_grad = (
            numbers[0] * gate * (numbers[5] + numbers[6] + slope_dot) + logit_grad * pull_tangent
        )
        even = jnp.arange(group_rows) % FRESH == 0
        by_first = [numbers[1 + place] * input_grad for place in range(FRESH)]
        by_first = [
            part + jnp.where(even, jnp.roll(part, -1), jnp.roll(part, 1)) for part in by_first
        ]
        return (
            jnp.where(even, by_first[0], by_first[1]),
            rows_cached + live * gate_own * change,
            value,
            pull,
            logit_grad,
            shards_of(columns_of(stacked[:group_rows])),
        )

    def first_waits():
        value_first, slope_first, gate_first, rows_cached, columns_first = state
        factor = live * gate_first * (1.0 - gate_first)
        factors = jnp.pad(jnp.concatenate(two_parts(factor), axis=1), ((0, 0), (0, 126)))
        rows = jnp.concatenate([r_out[None, :] * slope_first, value_first, factors], axis=1)
        rows = from_everyone(rows.astype(jnp.bfloat16), "fsdp_0").astype(jnp.float32)
        return (
            jnp.zeros((group_rows,), jnp.float32),
            rows_cached + passing[:, :features],
            rows[:, hidden : 2 * hidden],
            rows[:, :hidden],
            rows[:, 2 * hidden] + rows[:, 2 * hidden + 1],
            shards_of(columns_first),
        )

    returning, new_rows, value, pull, logit_grad, shards = lax.cond(
        second_section, second_part, first_waits
    )

    returned = lax.ppermute(returning, "pipe", [(1, 0)])
    flags = jnp.stack([second_section.astype(jnp.float32), timestep[0].astype(jnp.float32)])
    message = final_message(flags, returned, logit_grad, pull, value, shards, plane_count)
    arrived = lax.all_to_all(message, PLANE, split_axis=0, concat_axis=0, tiled=True)
    plane_rows = arrived[:, :group_rows].reshape(plane_count * group_rows, -1)
    hidden_rows = plane_rows[:, :hidden]
    summed_in = contract_first(plane_rows[:, hidden : hidden + shard_cols], hidden_rows)
    steps = jnp.arange(router_bias.shape[1]).astype(jnp.bfloat16)
    is_step = (steps[:, None] == arrived[:, group_rows + 1, 0][None, :]).astype(jnp.bfloat16)
    summed_bias = times(jnp.repeat(is_step, group_rows, axis=1), hidden_rows)
    summed_out = jnp.sum(arrived[:, group_rows, :hidden].astype(jnp.float32), axis=0)

    new_rows = new_rows.astype(jnp.bfloat16)
    blended = cached
    for row in range(FRESH):
        blended = jnp.where(picked[row][:, None] > 0, new_rows[row][None, :], blended)
    return (blended[None, None], summed_in[None], summed_bias[None], summed_out[None])


def solution(mesh):
    torus = Mesh(
        mesh.devices.reshape(16, 2, mesh.shape["pipe"], mesh.shape["dp"]),
        ("fsdp_0", "fsdp_1", "pipe", "dp"),
    )
    return jax.shard_map(
        body,
        mesh=torus,
        in_specs=(
            P("dp", FSDP, None),
            P("pipe", "dp", FSDP, None),
            P("pipe", "dp", FSDP),
            P("dp"),
            P("pipe", FSDP, None),
            P("pipe", FSDP, None),
            P("pipe", FSDP, None),
            P("pipe", None, None),
            P("pipe", None),
            P("dp", FSDP, None),
        ),
        out_specs=(
            P("pipe", "dp", FSDP, None),
            P("pipe", FSDP, None),
            P("pipe", None, None),
            P("pipe", None),
        ),
        check_vma=False,
    )
```

```python
import jax
import jax.numpy as jnp
from jax import lax
from jax.experimental import pallas as pl
from jax.experimental.pallas import tpu as pltpu
from jax.sharding import Mesh
from jax.sharding import PartitionSpec as P


FRESH = 2
FSDP = ("fsdp_0", "fsdp_1")
PLANE = ("fsdp_1", "dp")


layer_eps = 1e-06
gelu_scale = 0.7978845608028654
gelu_cubic = 0.044715


def from_everyone(value, axis):
    copies = jnp.broadcast_to(value, (lax.axis_size(axis), *value.shape))
    arrived = lax.all_to_all(copies, axis, split_axis=0, concat_axis=0, tiled=True)
    return arrived.reshape(-1, value.shape[-1])


def summed_on_arrival(value, axis):
    blocks = value.reshape(lax.axis_size(axis), -1, value.shape[-1])
    arrived = lax.all_to_all(blocks, axis, split_axis=0, concat_axis=0, tiled=True)
    return arrived.astype(jnp.float32).sum(axis=0)


def gelu_both(values):
    inner_arg = gelu_scale * (values + gelu_cubic * values * values * values)
    tanh_val = jnp.tanh(inner_arg)
    half = 0.5 * (1.0 + tanh_val)
    slope = half + 0.5 * values * (1.0 - tanh_val * tanh_val) * gelu_scale * (
        1.0 + 3.0 * gelu_cubic * values * values
    )
    return (values * half, slope)


def normalize(inputs):
    values = inputs.astype(jnp.float32)
    center = values - jnp.mean(values, axis=1, keepdims=True)
    inv_std = lax.rsqrt(jnp.mean(center * center, axis=1, keepdims=True) + layer_eps)
    return (center * inv_std, inv_std)


def contract_last(left, right):
    return lax.dot_general(
        left, right, (((1,), (1,)), ((), ())), preferred_element_type=jnp.float32
    )


def contract_first(left, right):
    return lax.dot_general(
        left, right, (((0,), (0,)), ((), ())), preferred_element_type=jnp.float32
    )


def times(left, right):
    return jnp.dot(left, right, preferred_element_type=jnp.float32)


def two_parts(values):
    upper = lax.reduce_precision(values, exponent_bits=8, mantissa_bits=7)
    return [upper, values - upper]


def unset(*arrays):
    return pl.pallas_call(
        lambda *refs: None,
        out_shape=[jax.ShapeDtypeStruct(shape, dtype) for shape, dtype in arrays],
        out_specs=[pl.BlockSpec(memory_space=pl.ANY)] * len(arrays),
    )()


def final_message(flags, returned, logit, pull, value, shards, plane_count):
    rows, hidden = pull.shape
    per_shard = plane_count // shards.shape[0]
    lanes = shards.shape[2]

    def kernel(flags_ref, returned_ref, logit_ref, pull_ref, value_ref, shards_ref, out_ref):
        square = [lax.broadcasted_iota(jnp.int32, (rows, rows), axis) for axis in (0, 1)]
        scale = jnp.where(square[0] == square[1], returned_ref[...], 0.0)
        scale = jnp.sum(scale, axis=1, keepdims=True)
        grads = logit_ref[...] * jnp.where(flags_ref[0] > 0, 1.0, scale)
        hidden_rows = (grads * pull_ref[...]).astype(jnp.bfloat16)
        out_row = jnp.sum(grads * value_ref[...], axis=0, keepdims=True)
        place = lax.broadcasted_iota(jnp.int32, (8, hidden), 0)
        tail = jnp.where(place == 0, out_row, jnp.where(place == 1, flags_ref[1], 0.0))
        tail = tail.astype(jnp.bfloat16)
        for target in range(plane_count):
            out_ref[target, :rows, :hidden] = hidden_rows
            out_ref[target, :rows, hidden:] = shards_ref[target // per_shard]
            out_ref[target, rows:, :hidden] = tail
            out_ref[target, rows:, hidden:] = jnp.zeros((8, lanes), jnp.bfloat16)

    vmem = pl.BlockSpec(memory_space=pltpu.VMEM)
    return pl.pallas_call(
        kernel,
        out_shape=jax.ShapeDtypeStruct((plane_count, rows + 8, hidden + lanes), jnp.bfloat16),
        in_specs=[pl.BlockSpec(memory_space=pltpu.SMEM)] + [vmem] * 5,
        out_specs=vmem,
    )(flags, returned[None], logit, pull, value, shards)


def pick_fresh(mask_row):
    rows = mask_row.shape[0]
    fresh = (mask_row > 0).astype(jnp.float32)
    before = (jnp.arange(rows)[:, None] <= jnp.arange(rows)[None, :]).astype(jnp.float32)
    rank = jnp.sum(before * fresh[:, None], axis=0)
    wanted = jnp.arange(1, FRESH + 1).astype(jnp.float32)
    return jnp.where(rank[None, :] == wanted[:, None], fresh[None, :], 0.0)


def rows_at(picked, values):
    return times(picked.astype(jnp.bfloat16), values)


def body(
    video_tokens,
    cached_out,
    fresh_mask,
    timestep,
    up_weight,
    down_weight,
    router_in,
    router_bias,
    router_out,
    out_cotangent,
):
    second_section = lax.axis_index("pipe") == 1
    near = lax.axis_index("fsdp_1")
    along = lax.axis_index("fsdp_0")
    column_slot = lax.axis_index(FSDP)
    cached = cached_out[0, 0]
    w_up = up_weight[0]
    w_down = down_weight[0]
    r_in = router_in[0]
    r_out = router_out[0]
    features = cached.shape[1]
    hidden = r_in.shape[1]
    shard_cols = r_in.shape[0]
    near_count = lax.axis_size("fsdp_1")
    along_count = lax.axis_size("fsdp_0")
    group_rows = along_count * FRESH
    dp_count = lax.axis_size("dp")
    plane_count = near_count * dp_count
    pair_cols = near_count * shard_cols
    bias_row = lax.dynamic_slice_in_dim(router_bias[0], timestep[0], 1)

    cached_before = lax.ppermute(cached, "pipe", [(0, 1)])
    picked = pick_fresh(fresh_mask[0, 0])
    live = jnp.sum(picked, axis=1, keepdims=True)

    def gate_of(router_pre):
        value, slope = gelu_both(router_pre)
        gate = jax.nn.sigmoid(jnp.sum(value * r_out[None, :], axis=1, keepdims=True))
        return (value, slope, gate)

    def columns_of(rows):
        return lax.dynamic_slice_in_dim(rows, along * pair_cols, pair_cols, 1)

    def from_next(value, section):
        place = lambda x_hi, dp: (x_hi * 2 + section) * dp_count + dp
        route = [
            (place(x_hi, dp), place(1 - x_hi, dp ^ (dp_count // 2)))
            for x_hi in range(near_count)
            for dp in range(dp_count)
        ]
        return lax.ppermute(value, ("fsdp_1", "pipe", "dp"), route)

    def up_both(rows, other_up):
        return jnp.concatenate([contract_last(rows, w_up), contract_last(rows, other_up)], axis=1)

    def down_both(act, other_down):
        act = act.astype(jnp.bfloat16)
        own_units = w_down.shape[0]
        return times(act[:, :own_units], w_down) + times(act[:, own_units:], other_down)

    def shards_of(columns):
        shards = jnp.moveaxis(columns.reshape(group_rows, near_count, shard_cols), 1, 0)
        return jnp.pad(shards, ((0, 0), (0, 0), (0, 128 - shard_cols)))

    def first_part():
        rows_first = rows_at(picked, video_tokens[0])
        rows_cached = rows_at(picked, cached)
        scaled_first, _ = normalize(rows_first)
        gathered = from_everyone(scaled_first.astype(jnp.bfloat16), FSDP)
        act_first, _ = gelu_both(contract_last(gathered, w_up))
        terms = times(act_first.astype(jnp.bfloat16), w_down)
        columns = lax.dynamic_slice_in_dim(gathered, column_slot * shard_cols, shard_cols, 1)
        sums_first = jnp.concatenate([terms, times(columns, r_in)], axis=1)
        sums_first = summed_on_arrival(sums_first.astype(jnp.bfloat16), FSDP)
        by_near = gathered.reshape(along_count, near_count, FRESH, features)
        group_first = lax.dynamic_index_in_dim(by_near, near, 1, keepdims=False)
        columns_first = columns_of(group_first.reshape(group_rows, features))
        value_first, slope_first, gate_first = gate_of(sums_first[:, features:] + bias_row)
        change_first = rows_first + sums_first[:, :features] - rows_cached
        added_first = live * gate_first * change_first
        nothing = unset(
            (w_up.shape, w_up.dtype),
            (w_down.shape, w_down.dtype),
            ((features, hidden), r_in.dtype),
            ((group_rows, near_count * w_down.shape[0]), jnp.float32),
            ((group_rows, features), jnp.bfloat16),
        )
        passing = jnp.concatenate([added_first, change_first, picked], axis=1)
        state = (value_first, slope_first, gate_first, rows_cached, columns_first)
        return (passing, state, rows_cached, tuple(nothing))

    def second_waits():
        cot_rows = rows_at(picked, out_cotangent[0])
        piece = shard_cols // dp_count
        own_piece = lax.dynamic_slice_in_dim(r_in, lax.axis_index("dp") * piece, piece)
        sent = jnp.concatenate([cot_rows.astype(jnp.bfloat16), own_piece.reshape(1, features)])
        sent = from_everyone(sent, "fsdp_0")
        sent = sent.reshape(along_count, FRESH + 1, features)
        group = sent[:, :FRESH].reshape(group_rows, features)
        pieces = sent[:, FRESH].reshape(along_count * piece, hidden)
        other_up = from_next(w_up, 1)
        other_down = from_next(w_down, 1)
        whole_in = from_everyone(pieces, PLANE)
        act_grad = jnp.concatenate(
            [contract_last(group, w_down), contract_last(group, other_down)], axis=1
        )
        row = jnp.zeros((FRESH, hidden), jnp.float32)
        (columns,) = unset(((group_rows, pair_cols), jnp.bfloat16))
        state = (row, row, row[:, :1], rows_at(picked, cached), columns)
        passing = jnp.zeros((FRESH, 2 * features + picked.shape[1]), jnp.float32)
        return (passing, state, cot_rows, (other_up, other_down, whole_in, act_grad, group))

    passing, state, cot, others = lax.cond(second_section, second_waits, first_part)
    passed = lax.ppermute(passing, "pipe", [(0, 1)])
    cached_asked = rows_at(picked, cached_before)

    def second_part():
        other_up, other_down, whole_in, act_grad, cot_group = others
        rows_cached = state[3]
        match = contract_last(picked, passed[:, 2 * features :])

        def at_match(values):
            return match[:, :1] * values[:1] + match[:, 1:] * values[1:]

        rows_second = cached_asked + at_match(passed[:, :features])
        rows_second = rows_second.astype(jnp.bfloat16).astype(jnp.float32)
        moved = at_match(passed[:, features : 2 * features])
        scaled, inv_std = normalize(rows_second)
        tangent = inv_std * (
            moved
            - jnp.mean(moved, axis=1, keepdims=True)
            - scaled * jnp.mean(moved * scaled, axis=1, keepdims=True)
        )
        standing = jnp.sum(cot * (rows_second - rows_cached), axis=1, keepdims=True)
        moving = jnp.sum(cot * moved, axis=1, keepdims=True)
        numbers = jnp.concatenate(
            [live, match, *two_parts(standing), *two_parts(moving)], axis=1
        )
        numbers = jnp.pad(numbers, ((0, 0), (0, 128 - numbers.shape[1])))
        both = jnp.concatenate([scaled, tangent, numbers], axis=1).astype(jnp.bfloat16)
        both = from_everyone(both, "fsdp_0")
        stacked = jnp.concatenate([both[:, :features], both[:, features : 2 * features]])
        numbers = both[:, 2 * features :].astype(jnp.float32)
        pre_both = up_both(stacked, other_up)
        act, act_slope = gelu_both(pre_both[:group_rows])
        terms = down_both(act, other_down)
        block_parts = jnp.sum(terms * cot_group.astype(jnp.float32), axis=1)
        slope_parts = jnp.sum(act_grad * act_slope * pre_both[group_rows:], axis=1)
        parts = jnp.pad(jnp.stack([block_parts, slope_parts]), ((0, 0), (0, 128 - group_rows)))
        parts = jnp.broadcast_to(parts.astype(jnp.bfloat16), (along_count, *parts.shape))
        terms = terms.astype(jnp.bfloat16).reshape(along_count, FRESH, features)
        sums = summed_on_arrival(jnp.concatenate([terms, parts], axis=2), "fsdp_0")

        piece = shard_cols // dp_count
        whole_in = whole_in.reshape(near_count, dp_count, along_count, piece, hidden)
        whole_in = whole_in.transpose(2, 0, 1, 3, 4).reshape(features, hidden)
        routed = times(stacked, whole_in)
        value, slope, gate = gate_of(routed[:group_rows] + bias_row)
        pull = r_out[None, :] * slope
        pull_tangent = jnp.sum(pull * routed[group_rows:], axis=1, keepdims=True)
        gate_own = lax.dynamic_slice_in_dim(gate, along * FRESH, FRESH)
        change = rows_second + sums[:, :features] - rows_cached
        live_group = numbers[:, :1]
        block_dot = sums[0, features : features + group_rows][:, None]
        slope_dot = sums[1, features : features + group_rows][:, None]
        gate_grad = live_group * (numbers[:, 3:4] + numbers[:, 4:5] + block_dot)
        logit_grad = gate_grad * gate * (1.0 - gate)
        input_grad = live_group * gate * (
            numbers[:, 5:6] + numbers[:, 6:7] + slope_dot
        ) + logit_grad * pull_tangent
        returning = (numbers[:, 1:3] * input_grad).reshape(along_count, FRESH, FRESH)
        return (
            jnp.sum(returning, axis=1).reshape(group_rows),
            rows_cached + live * gate_own * change,
            value,
            pull,
            logit_grad,
            shards_of(columns_of(stacked[:group_rows])),
        )

    def first_waits():
        value_first, slope_first, gate_first, rows_cached, columns_first = state
        factor = live * gate_first * (1.0 - gate_first)
        factors = jnp.pad(jnp.concatenate(two_parts(factor), axis=1), ((0, 0), (0, 126)))
        rows = jnp.concatenate([r_out[None, :] * slope_first, value_first, factors], axis=1)
        rows = from_everyone(rows.astype(jnp.bfloat16), "fsdp_0").astype(jnp.float32)
        return (
            jnp.zeros((group_rows,), jnp.float32),
            rows_cached + passing[:, :features],
            rows[:, hidden : 2 * hidden],
            rows[:, :hidden],
            rows[:, 2 * hidden : 2 * hidden + 1] + rows[:, 2 * hidden + 1 : 2 * hidden + 2],
            shards_of(columns_first),
        )

    returning, new_rows, value, pull, logit_grad, shards = lax.cond(
        second_section, second_part, first_waits
    )

    returned = lax.ppermute(returning, "pipe", [(1, 0)])
    flags = jnp.stack([second_section.astype(jnp.float32), timestep[0].astype(jnp.float32)])
    message = final_message(flags, returned, logit_grad, pull, value, shards, plane_count)
    arrived = lax.all_to_all(message, PLANE, split_axis=0, concat_axis=0, tiled=True)
    plane_rows = arrived[:, :group_rows].reshape(plane_count * group_rows, -1)
    hidden_rows = plane_rows[:, :hidden]
    summed_in = contract_first(plane_rows[:, hidden : hidden + shard_cols], hidden_rows)
    steps = jnp.arange(router_bias.shape[1]).astype(jnp.bfloat16)
    is_step = (steps[:, None] == arrived[:, group_rows + 1, 0][None, :]).astype(jnp.bfloat16)
    summed_bias = times(jnp.repeat(is_step, group_rows, axis=1), hidden_rows)
    summed_out = jnp.sum(arrived[:, group_rows, :hidden].astype(jnp.float32), axis=0)

    new_rows = new_rows.astype(jnp.bfloat16)
    blended = cached
    for row in range(FRESH):
        blended = jnp.where(picked[row][:, None] > 0, new_rows[row][None, :], blended)
    return (blended[None, None], summed_in[None], summed_bias[None], summed_out[None])


def solution(mesh):
    torus = Mesh(
        mesh.devices.reshape(16, 2, mesh.shape["pipe"], mesh.shape["dp"]),
        ("fsdp_0", "fsdp_1", "pipe", "dp"),
    )
    return jax.shard_map(
        body,
        mesh=torus,
        in_specs=(
            P("dp", FSDP, None),
            P("pipe", "dp", FSDP, None),
            P("pipe", "dp", FSDP),
            P("dp"),
            P("pipe", FSDP, None),
            P("pipe", FSDP, None),
            P("pipe", FSDP, None),
            P("pipe", None, None),
            P("pipe", None),
            P("dp", FSDP, None),
        ),
        out_specs=(
            P("pipe", "dp", FSDP, None),
            P("pipe", FSDP, None),
            P("pipe", None, None),
            P("pipe", None),
        ),
        check_vma=False,
    )
```

```python
import jax
import jax.numpy as jnp
from jax import lax
from jax.experimental import pallas as pl
from jax.experimental.pallas import tpu as pltpu
from jax.sharding import Mesh
from jax.sharding import PartitionSpec as P


FRESH = 2
FSDP = ("fsdp_0", "fsdp_1")
PLANE = ("fsdp_1", "dp")


layer_eps = 1e-06
gelu_scale = 0.7978845608028654
gelu_cubic = 0.044715


def from_everyone(value, axis):
    copies = jnp.broadcast_to(value, (lax.axis_size(axis), *value.shape))
    arrived = lax.all_to_all(copies, axis, split_axis=0, concat_axis=0, tiled=True)
    return arrived.reshape(-1, value.shape[-1])


def summed_on_arrival(value, axis):
    blocks = value.reshape(lax.axis_size(axis), -1, value.shape[-1])
    arrived = lax.all_to_all(blocks, axis, split_axis=0, concat_axis=0, tiled=True)
    return arrived.astype(jnp.float32).sum(axis=0)


def gelu_both(values):
    inner_arg = gelu_scale * (values + gelu_cubic * values * values * values)
    tanh_val = jnp.tanh(inner_arg)
    half = 0.5 * (1.0 + tanh_val)
    slope = half + 0.5 * values * (1.0 - tanh_val * tanh_val) * gelu_scale * (
        1.0 + 3.0 * gelu_cubic * values * values
    )
    return (values * half, slope)


def normalize(inputs):
    values = inputs.astype(jnp.float32)
    center = values - jnp.mean(values, axis=1, keepdims=True)
    inv_std = lax.rsqrt(jnp.mean(center * center, axis=1, keepdims=True) + layer_eps)
    return (center * inv_std, inv_std)


def contract_last(left, right):
    return lax.dot_general(
        left, right, (((1,), (1,)), ((), ())), preferred_element_type=jnp.float32
    )


def contract_first(left, right):
    return lax.dot_general(
        left, right, (((0,), (0,)), ((), ())), preferred_element_type=jnp.float32
    )


def times(left, right):
    return jnp.dot(left, right, preferred_element_type=jnp.float32)


def two_parts(values):
    upper = lax.reduce_precision(values, exponent_bits=8, mantissa_bits=7)
    return [upper, values - upper]


def unset(*arrays):
    return pl.pallas_call(
        lambda *refs: None,
        out_shape=[jax.ShapeDtypeStruct(shape, dtype) for shape, dtype in arrays],
        out_specs=[pl.BlockSpec(memory_space=pl.ANY)] * len(arrays),
    )()


def final_message(flags, returned, logit, pull, value, shards, plane_count):
    rows, hidden = pull.shape
    per_shard = plane_count // shards.shape[0]
    lanes = shards.shape[2]

    def kernel(flags_ref, returned_ref, logit_ref, pull_ref, value_ref, shards_ref, out_ref):
        square = [lax.broadcasted_iota(jnp.int32, (rows, rows), axis) for axis in (0, 1)]
        grads = logit_ref[...] * jnp.where(flags_ref[0] > 0, 1.0, returned_ref[...])
        grads = jnp.where(square[0] == square[1], grads, 0.0)
        grads = jnp.sum(grads, axis=1, keepdims=True)
        hidden_rows = (grads * pull_ref[...]).astype(jnp.bfloat16)
        out_row = jnp.sum(grads * value_ref[...], axis=0, keepdims=True)
        place = lax.broadcasted_iota(jnp.int32, (8, hidden), 0)
        tail = jnp.where(place == 0, out_row, jnp.where(place == 1, flags_ref[1], 0.0))
        tail = tail.astype(jnp.bfloat16)
        for target in range(plane_count):
            out_ref[target, :rows, :hidden] = hidden_rows
            out_ref[target, :rows, hidden:] = shards_ref[target // per_shard]
            out_ref[target, rows:, :hidden] = tail
            out_ref[target, rows:, hidden:] = jnp.zeros((8, lanes), jnp.bfloat16)

    vmem = pl.BlockSpec(memory_space=pltpu.VMEM)
    return pl.pallas_call(
        kernel,
        out_shape=jax.ShapeDtypeStruct((plane_count, rows + 8, hidden + lanes), jnp.bfloat16),
        in_specs=[pl.BlockSpec(memory_space=pltpu.SMEM)] + [vmem] * 5,
        out_specs=vmem,
    )(flags, returned[None], logit[None], pull, value, shards)


def pick_fresh(mask_row):
    rows = mask_row.shape[0]
    fresh = (mask_row > 0).astype(jnp.float32)
    before = (jnp.arange(rows)[:, None] <= jnp.arange(rows)[None, :]).astype(jnp.float32)
    rank = jnp.sum(before * fresh[:, None], axis=0)
    wanted = jnp.arange(1, FRESH + 1).astype(jnp.float32)
    return jnp.where(rank[None, :] == wanted[:, None], fresh[None, :], 0.0)


def rows_at(picked, values):
    return times(picked.astype(jnp.bfloat16), values)


def body(
    video_tokens,
    cached_out,
    fresh_mask,
    timestep,
    up_weight,
    down_weight,
    router_in,
    router_bias,
    router_out,
    out_cotangent,
):
    second_section = lax.axis_index("pipe") == 1
    near = lax.axis_index("fsdp_1")
    along = lax.axis_index("fsdp_0")
    column_slot = lax.axis_index(FSDP)
    cached = cached_out[0, 0]
    w_up = up_weight[0]
    w_down = down_weight[0]
    r_in = router_in[0]
    r_out = router_out[0]
    features = cached.shape[1]
    hidden = r_in.shape[1]
    shard_cols = r_in.shape[0]
    near_count = lax.axis_size("fsdp_1")
    along_count = lax.axis_size("fsdp_0")
    group_rows = along_count * FRESH
    dp_count = lax.axis_size("dp")
    plane_count = near_count * dp_count
    pair_cols = near_count * shard_cols
    bias_row = lax.dynamic_slice_in_dim(router_bias[0], timestep[0], 1)

    cached_before = lax.ppermute(cached, "pipe", [(0, 1)])
    picked = pick_fresh(fresh_mask[0, 0])
    live = jnp.sum(picked, axis=1, keepdims=True)

    def gate_of(router_pre):
        value, slope = gelu_both(router_pre)
        gate = jax.nn.sigmoid(jnp.sum(value * r_out[None, :], axis=1, keepdims=True))
        return (value, slope, gate)

    def columns_of(rows):
        return lax.dynamic_slice_in_dim(rows, along * pair_cols, pair_cols, 1)

    def from_next(value, section):
        place = lambda x_hi, dp: (x_hi * 2 + section) * dp_count + dp
        route = [
            (place(x_hi, dp), place(1 - x_hi, dp ^ (dp_count // 2)))
            for x_hi in range(near_count)
            for dp in range(dp_count)
        ]
        return lax.ppermute(value, ("fsdp_1", "pipe", "dp"), route)

    def up_both(rows, other_up):
        return jnp.concatenate([contract_last(rows, w_up), contract_last(rows, other_up)], axis=1)

    def down_both(act, other_down):
        act = act.astype(jnp.bfloat16)
        own_units = w_down.shape[0]
        return times(act[:, :own_units], w_down) + times(act[:, own_units:], other_down)

    def shards_of(columns):
        shards = jnp.moveaxis(columns.reshape(group_rows, near_count, shard_cols), 1, 0)
        return jnp.pad(shards, ((0, 0), (0, 0), (0, 128 - shard_cols)))

    def first_part():
        rows_first = rows_at(picked, video_tokens[0])
        rows_cached = rows_at(picked, cached)
        scaled_first, _ = normalize(rows_first)
        gathered = from_everyone(scaled_first.astype(jnp.bfloat16), FSDP)
        act_first, _ = gelu_both(contract_last(gathered, w_up))
        terms = times(act_first.astype(jnp.bfloat16), w_down)
        columns = lax.dynamic_slice_in_dim(gathered, column_slot * shard_cols, shard_cols, 1)
        sums_first = jnp.concatenate([terms, times(columns, r_in)], axis=1)
        sums_first = summed_on_arrival(sums_first.astype(jnp.bfloat16), FSDP)
        by_near = gathered.reshape(along_count, near_count, FRESH, features)
        group_first = lax.dynamic_index_in_dim(by_near, near, 1, keepdims=False)
        columns_first = columns_of(group_first.reshape(group_rows, features))
        value_first, slope_first, gate_first = gate_of(sums_first[:, features:] + bias_row)
        change_first = rows_first + sums_first[:, :features] - rows_cached
        added_first = live * gate_first * change_first
        nothing = unset(
            (w_up.shape, w_up.dtype),
            (w_down.shape, w_down.dtype),
            ((features, hidden), r_in.dtype),
            ((group_rows, near_count * w_down.shape[0]), jnp.float32),
            ((group_rows, features), jnp.bfloat16),
        )
        passing = jnp.concatenate([added_first, change_first, picked], axis=1)
        state = (value_first, slope_first, gate_first, rows_cached, columns_first)
        return (passing, state, rows_cached, tuple(nothing))

    def second_waits():
        cot_rows = rows_at(picked, out_cotangent[0])
        piece = shard_cols // dp_count
        own_piece = lax.dynamic_slice_in_dim(r_in, lax.axis_index("dp") * piece, piece)
        pieces = from_everyone(own_piece.reshape(1, features), "fsdp_0")
        pieces = pieces.reshape(along_count * piece, hidden)
        group = from_everyone(cot_rows.astype(jnp.bfloat16), "fsdp_0")
        other_up = from_next(w_up, 1)
        other_down = from_next(w_down, 1)
        whole_in = from_everyone(pieces, PLANE)
        act_grad = jnp.concatenate(
            [contract_last(group, w_down), contract_last(group, other_down)], axis=1
        )
        row = jnp.zeros((FRESH, hidden), jnp.float32)
        (columns,) = unset(((group_rows, pair_cols), jnp.bfloat16))
        state = (row, row, row[:, :1], rows_at(picked, cached), columns)
        passing = jnp.zeros((FRESH, 2 * features + picked.shape[1]), jnp.float32)
        return (passing, state, cot_rows, (other_up, other_down, whole_in, act_grad, group))

    passing, state, cot, others = lax.cond(second_section, second_waits, first_part)
    passed = lax.ppermute(passing, "pipe", [(0, 1)])
    cached_asked = rows_at(picked, cached_before)

    def second_part():
        other_up, other_down, whole_in, act_grad, cot_group = others
        rows_cached = state[3]
        match = contract_last(picked, passed[:, 2 * features :])

        def at_match(values):
            return match[:, :1] * values[:1] + match[:, 1:] * values[1:]

        rows_second = cached_asked + at_match(passed[:, :features])
        rows_second = rows_second.astype(jnp.bfloat16).astype(jnp.float32)
        moved = at_match(passed[:, features : 2 * features])
        scaled, inv_std = normalize(rows_second)
        tangent = inv_std * (
            moved
            - jnp.mean(moved, axis=1, keepdims=True)
            - scaled * jnp.mean(moved * scaled, axis=1, keepdims=True)
        )
        standing = jnp.sum(cot * (rows_second - rows_cached), axis=1, keepdims=True)
        moving = jnp.sum(cot * moved, axis=1, keepdims=True)
        numbers = jnp.concatenate(
            [live, match, *two_parts(standing), *two_parts(moving)], axis=1
        )
        numbers = jnp.pad(numbers, ((0, 0), (0, 128 - numbers.shape[1])))
        both = jnp.concatenate([scaled, tangent, numbers], axis=1).astype(jnp.bfloat16)
        both = from_everyone(both, "fsdp_0")
        stacked = jnp.concatenate([both[:, :features], both[:, features : 2 * features]])
        numbers = both[:, 2 * features :].astype(jnp.float32)
        pre_both = up_both(stacked, other_up)
        act, act_slope = gelu_both(pre_both[:group_rows])
        terms = down_both(act, other_down)
        block_parts = jnp.sum(terms * cot_group.astype(jnp.float32), axis=1)
        slope_parts = jnp.sum(act_grad * act_slope * pre_both[group_rows:], axis=1)
        parts = jnp.pad(jnp.stack([block_parts, slope_parts]), ((0, 0), (0, 128 - group_rows)))
        parts = jnp.broadcast_to(parts.astype(jnp.bfloat16), (along_count, *parts.shape))
        terms = terms.astype(jnp.bfloat16).reshape(along_count, FRESH, features)
        sums = summed_on_arrival(jnp.concatenate([terms, parts], axis=2), "fsdp_0")

        piece = shard_cols // dp_count
        whole_in = whole_in.reshape(near_count, dp_count, along_count, piece, hidden)
        whole_in = whole_in.transpose(2, 0, 1, 3, 4).reshape(features, hidden)
        routed = times(stacked, whole_in)
        value, slope, gate = gate_of(routed[:group_rows] + bias_row)
        pull = r_out[None, :] * slope
        pull_tangent = jnp.sum(pull * routed[group_rows:], axis=1, keepdims=True)
        gate_own = lax.dynamic_slice_in_dim(gate, along * FRESH, FRESH)
        change = rows_second + sums[:, :features] - rows_cached
        live_group = numbers[:, :1]
        block_dot = sums[0, features : features + group_rows][:, None]
        slope_dot = sums[1, features : features + group_rows][:, None]
        gate_grad = live_group * (numbers[:, 3:4] + numbers[:, 4:5] + block_dot)
        logit_grad = gate_grad * gate * (1.0 - gate)
        input_grad = live_group * gate * (
            numbers[:, 5:6] + numbers[:, 6:7] + slope_dot
        ) + logit_grad * pull_tangent
        returning = (numbers[:, 1:3] * input_grad).reshape(along_count, FRESH, FRESH)
        return (
            jnp.sum(returning, axis=1).reshape(group_rows),
            rows_cached + live * gate_own * change,
            value,
            pull,
            logit_grad[:, 0],
            shards_of(columns_of(stacked[:group_rows])),
        )

    def first_waits():
        value_first, slope_first, gate_first, rows_cached, columns_first = state
        factor = live * gate_first * (1.0 - gate_first)
        factors = jnp.pad(jnp.concatenate(two_parts(factor), axis=1), ((0, 0), (0, 126)))
        rows = jnp.concatenate([r_out[None, :] * slope_first, value_first, factors], axis=1)
        rows = from_everyone(rows.astype(jnp.bfloat16), "fsdp_0").astype(jnp.float32)
        return (
            jnp.zeros((group_rows,), jnp.float32),
            rows_cached + passing[:, :features],
            rows[:, hidden : 2 * hidden],
            rows[:, :hidden],
            rows[:, 2 * hidden] + rows[:, 2 * hidden + 1],
            shards_of(columns_first),
        )

    returning, new_rows, value, pull, logit_grad, shards = lax.cond(
        second_section, second_part, first_waits
    )

    returned = lax.ppermute(returning, "pipe", [(1, 0)])
    flags = jnp.stack([second_section.astype(jnp.float32), timestep[0].astype(jnp.float32)])
    message = final_message(flags, returned, logit_grad, pull, value, shards, plane_count)
    arrived = lax.all_to_all(message, PLANE, split_axis=0, concat_axis=0, tiled=True)
    plane_rows = arrived[:, :group_rows].reshape(plane_count * group_rows, -1)
    hidden_rows = plane_rows[:, :hidden]
    summed_in = contract_first(plane_rows[:, hidden : hidden + shard_cols], hidden_rows)
    steps = jnp.arange(router_bias.shape[1]).astype(jnp.bfloat16)
    is_step = (steps[:, None] == arrived[:, group_rows + 1, 0][None, :]).astype(jnp.bfloat16)
    summed_bias = times(jnp.repeat(is_step, group_rows, axis=1), hidden_rows)
    summed_out = jnp.sum(arrived[:, group_rows, :hidden].astype(jnp.float32), axis=0)

    new_rows = new_rows.astype(jnp.bfloat16)
    blended = cached
    for row in range(FRESH):
        blended = jnp.where(picked[row][:, None] > 0, new_rows[row][None, :], blended)
    return (blended[None, None], summed_in[None], summed_bias[None], summed_out[None])


def solution(mesh):
    torus = Mesh(
        mesh.devices.reshape(16, 2, mesh.shape["pipe"], mesh.shape["dp"]),
        ("fsdp_0", "fsdp_1", "pipe", "dp"),
    )
    return jax.shard_map(
        body,
        mesh=torus,
        in_specs=(
            P("dp", FSDP, None),
            P("pipe", "dp", FSDP, None),
            P("pipe", "dp", FSDP),
            P("dp"),
            P("pipe", FSDP, None),
            P("pipe", FSDP, None),
            P("pipe", FSDP, None),
            P("pipe", None, None),
            P("pipe", None),
            P("dp", FSDP, None),
        ),
        out_specs=(
            P("pipe", "dp", FSDP, None),
            P("pipe", FSDP, None),
            P("pipe", None, None),
            P("pipe", None),
        ),
        check_vma=False,
    )
```
